768 devices in a mesh: gx: 24 (over x, z_hi, core), gy: 8 (over y), gz: 4 (over z_lo).
Axes of the slice: x: 4, y: 8, z: 12 (z_hi: 3, z_lo: 4; z = z_hi * 4 + z_lo), core: 2. Of those that a mesh axis runs over, the one named last changes fastest.
Arguments:
- fields: float32 [32, 192, 64, 512], P(None, 'gx', 'gy', 'gz'), may hold values from -8 to 8
- strength: float32 [32], replicated, may hold values from 0.3 to 1
Outputs:
- filtered: float32 [32, 192, 64, 512], P(None, 'gx', 'gy', 'gz')
The draws below stay inside these ranges and needn't reach their ends.
All inputs are finite; a program needn't handle non-finite values.
Results may differ from the reference program's by a relative error of at most 0.00002.
Values sent between devices are 32-bit elements; how exact they have to be, the bound alone decides.
A program may use at most 64 MiB of HBM per device.

```python
import math
import jax
import jax.numpy as jnp
from jax import lax

SPECIES = 32
NX = 192
NY = 64
NZ = 512


def steps_of(own_key, extent, shards, smallest, top_value):
    def one(axis_at, shards_of):
        draws = jax.random.uniform(jax.random.fold_in(jax.random.fold_in(own_key, 6), axis_at), (shards_of,), jnp.float32, smallest / len(shards), top_value / len(shards))
        return jnp.repeat(jnp.exp(draws), extent[axis_at] // shards_of).reshape((-1,) + (1,) * (len(extent) - axis_at - 1))

    gain = one(*shards[0])
    for cut in shards[1:]:
        gain = gain * one(*cut)
    return gain


def scatter_about(own_key, shape, scale, reach, split=(), kind=jnp.bfloat16):
    values = jax.random.normal(own_key, shape, jnp.float32) * scale
    if len(split) > 0:
        values = steps_of(own_key, shape, split, -0.22, 0.18) * values
    return jnp.clip(values, min=-reach, max=reach).astype(kind)


def setup_inputs(seed: int = 0) -> dict:
    key_of = jax.random.split(jax.random.key(seed), 3)
    fields = scatter_about(key_of[0], (SPECIES, NX, NY, NZ), 1.0, 8.0, ((1, 24), (2, 8), (3, 4)), jnp.float32)
    strength = jnp.clip(jnp.exp(jax.random.uniform(key_of[1], (SPECIES,), jnp.float32, math.log(0.3), math.log(1.0))), 0.3, 1.0)
    return {"fields": fields, "strength": strength}


filter_weights = [1.0, -10.0, 45.0, -120.0, 210.0, -252.0, 210.0, -120.0, 45.0, -10.0, 1.0]


def tenth_difference(field, axis):
    total = jnp.zeros(field.shape, jnp.float32)
    for index in range(11):
        total = total + filter_weights[index] * jnp.roll(field, 5 - index, axis)
    return total


def filter_species(packed):
    field, scale = packed
    summed = tenth_difference(field, 0) + tenth_difference(field, 1) + tenth_difference(field, 2)
    return field + (scale / 1024.0) * summed


def reference(fields, strength):
    return lax.map(filter_species, (fields, strength))
```

```python
import functools

import jax
import jax.numpy as jnp
from jax import lax
from jax.experimental import pallas as pl
from jax.experimental.pallas import tpu as pltpu
from jax.sharding import PartitionSpec as P

MESH = pl.DeviceIdType.MESH

center = -252.0
weights = (210.0, -120.0, 45.0, -10.0, 1.0)
reach = 5

Z_GROUPS = 3
chunks = 8
relays = 3


def tap_sum(tiles, length):
    out = []
    for i in range(length):
        total = center * tiles[i + reach]
        for k in range(1, reach + 1):
            total = total + weights[k - 1] * (tiles[i + reach - k] + tiles[i + reach + k])
        out.append(total)
    return out


def kernel(
    sizes,
    fields,
    strength,
    out,
    xp,
    yt,
    acc,
    hold,
    zs,
    zr,
    scale,
    load_sem,
    scale_sem,
    x_send,
    hold_recv,
    far_recv,
    near_send,
    near_recv,
    y_send,
    y_recv,
    z_send,
    z_recv,
):
    nx, ny, nz = sizes
    species = xp.shape[0]
    cells = fields.shape[1]
    per = species // chunks
    pairs = species // 2

    gx = lax.axis_index("gx")
    gy = lax.axis_index("gy")
    gz = lax.axis_index("gz")
    core = lax.rem(gx, 2)
    chip = lax.div(gx, 2)
    z_hi = lax.rem(chip, Z_GROUPS)
    chip_x = lax.div(chip, Z_GROUPS)
    x_count = nx // (2 * Z_GROUPS)
    z_count = Z_GROUPS * nz
    z = z_hi * nz + gz
    step = 2 * core - 1

    def place(at_x, at_z, at_core):
        at_z = lax.rem(at_z + 2 * z_count, z_count)
        at_x = lax.rem(at_x + x_count, x_count)
        hi = lax.div(at_z, nz)
        return {"gx": (at_x * Z_GROUPS + hi) * 2 + at_core, "gz": lax.rem(at_z, nz)}

    edge = jnp.where(core == 1, Z_GROUPS - 1, 0)
    relay_to = place(chip_x, z + step, core)
    relay_from = place(chip_x, z - step, core)
    origin = lax.div(lax.rem(z - 3 * step + 2 * z_count, z_count), nz)
    last_to = place(jnp.where(origin == edge, chip_x + step, chip_x), z + step, 1 - core)
    back = -step
    before = lax.div(lax.rem(z - 4 * back + 2 * z_count, z_count), nz)
    back_edge = jnp.where(core == 1, 0, Z_GROUPS - 1)
    last_from = place(jnp.where(before == back_edge, chip_x - back, chip_x), z - back, 1 - core)
    partner = {"gx": chip * 2 + 1 - core}
    y_up = {"gy": lax.rem(gy + 1, ny)}
    y_down = {"gy": lax.rem(gy + ny - 1, ny)}
    z_up = {"gz": lax.rem(gz + 1, nz)}
    z_down = {"gz": lax.rem(gz + nz - 1, nz)}

    barrier = pltpu.get_barrier_semaphore()
    for who in (relay_from, last_from, partner, y_up, y_down, z_up, z_down):
        pl.semaphore_signal(barrier, inc=1, device_id=who, device_id_type=MESH)

    def load(j):
        return pltpu.make_async_copy(
            fields.at[pl.ds(j * per, per)], xp.at[pl.ds(j * per, per), pl.ds(reach, cells)], load_sem.at[j]
        )

    for j in range(chunks):
        load(j).start()
    scale_copy = pltpu.make_async_copy(strength, scale, scale_sem)
    scale_copy.start()
    for j in range(chunks):
        load(j).wait()

    def pack(p, _):
        block = xp[pl.ds(2 * p, 2), pl.ds(reach, cells)].reshape(128, 128)
        turned = jnp.transpose(block)
        zs[0, p] = turned[0:8]
        zs[1, p] = turned[120:128]
        return 0

    lax.fori_loop(0, pairs, pack, 0)

    pl.semaphore_wait(barrier, 7)

    away = reach + (cells - reach) * core
    arrive = (reach + cells) * (1 - core)

    def first_hop(j):
        return pltpu.make_async_remote_copy(
            src_ref=xp.at[pl.ds(j * per, per), pl.ds(away, reach)],
            dst_ref=hold.at[0, pl.ds(j * per, per)],
            send_sem=x_send.at[0, j],
            recv_sem=hold_recv.at[0, j],
            device_id=relay_to,
            device_id_type=MESH,
        )

    def mid_hop(h, j):
        return pltpu.make_async_remote_copy(
            src_ref=hold.at[h - 1, pl.ds(j * per, per)],
            dst_ref=hold.at[h, pl.ds(j * per, per)],
            send_sem=x_send.at[h, j],
            recv_sem=hold_recv.at[h, j],
            device_id=relay_to,
            device_id_type=MESH,
        )

    def last_hop(j):
        return pltpu.make_async_remote_copy(
            src_ref=hold.at[relays - 1, pl.ds(j * per, per)],
            dst_ref=xp.at[pl.ds(j * per, per), pl.ds((reach + cells) * (1 - core), reach)],
            send_sem=x_send.at[relays, j],
            recv_sem=far_recv.at[j],
            device_id=last_to,
            device_id_type=MESH,
        )

    def last_hop_in(j):
        return pltpu.make_async_remote_copy(
            src_ref=hold.at[relays - 1, pl.ds(j * per, per)],
            dst_ref=xp.at[pl.ds(j * per, per), pl.ds((reach + cells) * core, reach)],
            send_sem=x_send.at[relays, j],
            recv_sem=far_recv.at[j],
            device_id=last_to,
            device_id_type=MESH,
        )

    near = pltpu.make_async_remote_copy(
        src_ref=xp.at[:, pl.ds(reach + (cells - reach) * (1 - core), reach)],
        dst_ref=xp.at[:, pl.ds((reach + cells) * core, reach)],
        send_sem=near_send,
        recv_sem=near_recv,
        device_id=partner,
        device_id_type=MESH,
    )

    def z_copy(side, to):
        return pltpu.make_async_remote_copy(
            src_ref=zs.at[side],
            dst_ref=zr.at[side],
            send_sem=z_send.at[side],
            recv_sem=z_recv.at[side],
            device_id=to,
            device_id_type=MESH,
        )

    y_first = pltpu.make_async_remote_copy(
        src_ref=yt.at[:, pl.ds(reach, reach)],
        dst_ref=yt.at[:, pl.ds(reach + cells, reach)],
        send_sem=y_send.at[0],
        recv_sem=y_recv.at[0],
        device_id=y_down,
        device_id_type=MESH,
    )
    y_last = pltpu.make_async_remote_copy(
        src_ref=yt.at[:, pl.ds(cells, reach)],
        dst_ref=yt.at[:, pl.ds(0, reach)],
        send_sem=y_send.at[1],
        recv_sem=y_recv.at[1],
        device_id=y_up,
        device_id_type=MESH,
    )

    for j in range(chunks):
        first_hop(j).start()
    z_low = z_copy(0, z_down)
    z_high = z_copy(1, z_up)
    z_low.start()
    z_high.start()
    near.start()

    def turn(s, _):
        yt[s, pl.ds(reach, cells)] = jnp.swapaxes(xp[s, pl.ds(reach, cells)], 0, 1)
        return 0

    lax.fori_loop(0, species, turn, 0)
    y_first.start()
    y_last.start()

    z_low.wait()
    z_high.wait()
    lane = lax.broadcasted_iota(jnp.int32, (8, 128), 1)

    def z_sum(p, _):
        edges = jnp.concatenate([zr[0, p], jnp.zeros((112, 128), jnp.float32), zr[1, p]], axis=0)
        beside = jnp.transpose(edges)
        for half in range(2):
            for x in range(8):
                row = half * 8 + x
                own = xp[2 * p + half, reach + x]
                other = beside[row * 8 : row * 8 + 8]
                total = center * own
                for k in range(1, reach + 1):
                    left = pltpu.roll(jnp.where(lane >= 128 - k, other, own), k, 1)
                    right = pltpu.roll(jnp.where(lane < k, other, own), 128 - k, 1)
                    total = total + weights[k - 1] * (left + right)
                acc[2 * p + half, x] = total
        return 0

    lax.fori_loop(0, pairs, z_sum, 0)

    for j in range(chunks):
        first_hop(j).wait_recv()
        mid_hop(1, j).start()

    for j in range(chunks):
        mid_hop(1, j).wait_recv()
        mid_hop(2, j).start()

    y_first.wait()
    y_last.wait()

    def y_sum(s, _):
        tiles = [yt[s, i] for i in range(cells + 2 * reach)]
        total = jnp.stack(tap_sum(tiles, cells), axis=0)
        acc[s] = acc[s] + jnp.swapaxes(total, 0, 1)
        return 0

    lax.fori_loop(0, species, y_sum, 0)

    for j in range(chunks):
        mid_hop(2, j).wait_recv()
        last_hop(j).start()

    near.wait()
    scale_copy.wait()

    for j in range(chunks):
        last_hop_in(j).wait_recv()

        def finish(i, _):
            s = j * per + i
            tiles = [xp[s, i] for i in range(cells + 2 * reach)]
            total = tap_sum(tiles, cells)
            factor = scale[s] * (1.0 / 1024.0)
            for x in range(cells):
                out[s, x] = tiles[reach + x] + factor * (total[x] + acc[s, x])
            return 0

        lax.fori_loop(0, per, finish, 0)

    for j in range(chunks):
        first_hop(j).wait_send()
        mid_hop(1, j).wait_send()
        mid_hop(2, j).wait_send()
        last_hop(j).wait_send()


def local(sizes, fields, strength):
    species, cells, rows, lanes = fields.shape
    return pl.pallas_call(
        functools.partial(kernel, sizes),
        out_shape=jax.ShapeDtypeStruct(fields.shape, fields.dtype),
        in_specs=[pl.BlockSpec(memory_space=pl.ANY), pl.BlockSpec(memory_space=pl.ANY)],
        out_specs=pl.BlockSpec(memory_space=pltpu.VMEM),
        scratch_shapes=[
            pltpu.VMEM((species, cells + 2 * reach, rows, lanes), jnp.float32),
            pltpu.VMEM((species, rows + 2 * reach, cells, lanes), jnp.float32),
            pltpu.VMEM((species, cells, rows, lanes), jnp.float32),
            pltpu.VMEM((relays, species, reach, rows, lanes), jnp.float32),
            pltpu.VMEM((2, species // 2, 8, 128), jnp.float32),
            pltpu.VMEM((2, species // 2, 8, 128), jnp.float32),
            pltpu.SMEM((species,), jnp.float32),
            pltpu.SemaphoreType.DMA((chunks,)),
            pltpu.SemaphoreType.DMA,
            pltpu.SemaphoreType.DMA((relays + 1, chunks)),
            pltpu.SemaphoreType.DMA((relays, chunks)),
            pltpu.SemaphoreType.DMA((chunks,)),
            pltpu.SemaphoreType.DMA,
            pltpu.SemaphoreType.DMA,
            pltpu.SemaphoreType.DMA((2,)),
            pltpu.SemaphoreType.DMA((2,)),
            pltpu.SemaphoreType.DMA((2,)),
            pltpu.SemaphoreType.DMA((2,)),
        ],
        compiler_params=pltpu.CompilerParams(collective_id=0, has_side_effects=True),
    )(fields, strength)


def solution(mesh):
    sizes = (mesh.shape["gx"], mesh.shape["gy"], mesh.shape["gz"])
    return jax.shard_map(
        functools.partial(local, sizes),
        mesh=mesh,
        in_specs=(P(None, "gx", "gy", "gz"), P()),
        out_specs=P(None, "gx", "gy", "gz"),
        check_vma=False,
    )
```

```python
import functools

import jax
import jax.numpy as jnp
from jax import lax
from jax.experimental import pallas as pl
from jax.experimental.pallas import tpu as pltpu
from jax.sharding import PartitionSpec as P

MESH = pl.DeviceIdType.MESH

center = -252.0
weights = (210.0, -120.0, 45.0, -10.0, 1.0)
reach = 5

Z_GROUPS = 3
chunks = 8
relays = 3
detour = 1


def tap_sum(tiles, length):
    out = []
    for i in range(length):
        total = center * tiles[i + reach]
        for k in range(1, reach + 1):
            total = total + weights[k - 1] * (tiles[i + reach - k] + tiles[i + reach + k])
        out.append(total)
    return out


def kernel(
    sizes,
    fields,
    strength,
    out,
    xp,
    yt,
    zt,
    acc,
    hold,
    edge,
    beside,
    round_z,
    scale,
    load_sem,
    scale_sem,
    x_send,
    detour_send,
    hold_recv,
    detour_recv,
    far_recv,
    near_send,
    near_recv,
    y_send,
    y_recv,
    z_send,
    z_recv,
    round_recv,
    round_go,
):
    nx, ny, nz = sizes
    species = xp.shape[0]
    cells = fields.shape[1]
    per = species // chunks
    pairs = species // 2
    x_count = nx // (2 * Z_GROUPS)
    first = 2 * per

    gx = lax.axis_index("gx")
    gy = lax.axis_index("gy")
    gz = lax.axis_index("gz")

    chip = lax.div(gx, 2)
    core = gx - 2 * chip
    chip_x = lax.div(chip, Z_GROUPS)
    z_hi = chip - Z_GROUPS * chip_x
    upward = core == 1
    downward = core == 0
    step = 2 * core - 1

    def wrap(v, n):
        return jnp.where(v < 0, v + n, jnp.where(v >= n, v - n, v))

    def along(d):
        lo = gz + d
        carry = jnp.where(lo < 0, -1, jnp.where(lo >= nz, 1, 0))
        return wrap(z_hi + carry, Z_GROUPS), lo - carry * nz

    def place(at_x, hi, lo, at_core):
        return {"gx": (at_x * Z_GROUPS + hi) * 2 + at_core, "gz": lo}

    ahead = along(step)
    behind = along(-step)
    crosses = jnp.where(upward, ahead[0] == 0, ahead[0] == Z_GROUPS - 1)
    relay_to = place(chip_x, *ahead, core)
    relay_from = place(chip_x, *behind, core)
    last_to = place(wrap(chip_x + jnp.where(crosses, step, 0), x_count), *ahead, 1 - core)
    crossed = jnp.where(upward, z_hi == Z_GROUPS - 1, z_hi == 0)
    last_from = place(wrap(chip_x + jnp.where(crossed, step, 0), x_count), *ahead, 1 - core)
    partner = {"gx": chip * 2 + 1 - core}
    y_up = {"gy": wrap(gy + 1, ny)}
    y_down = {"gy": wrap(gy - 1, ny)}
    z_up = {"gz": wrap(gz + 1, nz)}
    z_down = {"gz": wrap(gz - 1, nz)}
    has_up = gz < nz - 1
    has_down = gz > 0
    near_ahead = jnp.where(upward, gz < nz - 1, gz > 0)
    near_behind = jnp.where(upward, gz > 0, gz < nz - 1)

    bottom, middle, top = 0, Z_GROUPS - 2, Z_GROUPS - 1
    round_from = jnp.where(upward, top, bottom)
    round_to = top - round_from
    sends_round = z_hi == round_from
    turns_round = z_hi == middle
    beyond = wrap(chip_x + step, x_count) * Z_GROUPS
    round_mid = {"gx": (chip_x * Z_GROUPS + middle) * 2 + core}
    round_source = {"gx": (chip_x * Z_GROUPS + round_from) * 2 + core}
    round_end = {"gx": (beyond + round_to) * 2 + 1 - core}
    round_turn = {"gx": (beyond + middle) * 2 + 1 - core}

    def skips(h):
        below = jnp.where(gz < h, wrap(z_hi - 1, Z_GROUPS), z_hi)
        above = jnp.where(gz + h >= nz, wrap(z_hi + 1, Z_GROUPS), z_hi)
        return jnp.where(upward, below, above) == round_from

    barrier = pltpu.get_barrier_semaphore()

    def greet(who):
        pl.semaphore_signal(barrier, inc=1, device_id=who, device_id_type=MESH)

    for who in (relay_from, last_from, partner, y_up, y_down):
        greet(who)

    @pl.when(near_ahead)
    def _():
        greet(relay_to)

    @pl.when(upward & turns_round)
    def _():
        greet(round_source)

    @pl.when(downward & turns_round)
    def _():
        greet(round_end)

    @pl.when(downward & sends_round)
    def _():
        greet(round_mid)
        greet(round_turn)

    greeted = 5 + jnp.where(near_behind, 1, 0) + jnp.where(turns_round, 1, jnp.where(upward & sends_round, 2, 0))

    loads = [
        pltpu.make_async_copy(fields.at[pl.ds(at, n)], xp.at[pl.ds(at, n), pl.ds(reach, cells)], load_sem.at[i])
        for i, (at, n) in enumerate(((0, first), (first, species - first)))
    ]
    for copy in loads:
        copy.start()
    scale_copy = pltpu.make_async_copy(strength, scale, scale_sem)
    scale_copy.start()

    def part(j):
        return pl.ds(j * per, per)

    def remote(src, dst, send, recv, to):
        return pltpu.make_async_remote_copy(
            src_ref=src, dst_ref=dst, send_sem=send, recv_sem=recv, device_id=to, device_id_type=MESH
        )

    far_there = (reach + cells) * (1 - core)
    far_here = (reach + cells) * core

    def away(j):
        return xp.at[part(j), pl.ds(reach + (cells - reach) * core, reach)]

    def hop(h, j):
        src = away(j) if h == 0 else hold.at[h - 1, part(j)]
        send = detour_send.at[h] if j < detour else x_send
        if h < relays:
            return remote(src, hold.at[h, part(j)], send, hold_recv.at[h, j], relay_to)
        return remote(src, xp.at[part(j), pl.ds(far_there, reach)], send, far_recv.at[j], last_to)

    def arrival(j):
        return remote(hold.at[0, part(j)], xp.at[part(j), pl.ds(far_here, reach)], x_send, far_recv.at[j], last_to)

    around = pl.ds(0, detour * per)

    def round_first():
        src = xp.at[around, pl.ds(reach + (cells - reach) * core, reach)]
        return remote(src, hold.at[relays, around], detour_send.at[0], detour_recv, round_mid)

    def round_last():
        dst = xp.at[around, pl.ds(far_there, reach)]
        return remote(hold.at[relays, around], dst, detour_send.at[relays + 1], far_recv.at[0], round_end)

    near = remote(
        xp.at[:, pl.ds(reach + (cells - reach) * (1 - core), reach)],
        xp.at[:, pl.ds(far_here, reach)],
        near_send,
        near_recv,
        partner,
    )
    y_copies = (
        remote(yt.at[:, pl.ds(reach, reach)], yt.at[:, pl.ds(reach + cells, reach)], y_send, y_recv, y_down),
        remote(yt.at[:, pl.ds(cells, reach)], yt.at[:, pl.ds(0, reach)], y_send, y_recv, y_up),
    )
    y_both = remote(yt.at[:, pl.ds(0, 2 * reach)], yt.at[:, pl.ds(0, 2 * reach)], y_send, y_recv, y_up)

    z_first, z_last = edge.at[0], edge.at[1]
    z_before, z_after = beside.at[0], beside.at[1]
    z_both = remote(beside, beside, z_send.at[0], z_recv, z_up)
    z_sent = [remote(edge, edge, z_send.at[i], z_recv, z_up) for i in range(2)]

    def go_up(src, dst, recv):
        return remote(src, dst, z_send.at[0], recv, z_up)

    def go_down(src, dst, recv):
        return remote(src, dst, z_send.at[1], recv, z_down)

    def z_start():
        @pl.when(has_up)
        def _():
            go_up(z_last, z_before, z_recv).start()

        @pl.when(has_down)
        def _():
            go_down(z_first, z_after, z_recv).start()

        @pl.when(gz == 0)
        def _():
            go_up(z_first, round_z.at[1], round_recv.at[1]).start()

        @pl.when(gz == nz - 1)
        def _():
            go_down(z_last, round_z.at[0], round_recv.at[0]).start()

    def z_pass():
        @pl.when(gz == 1)
        def _():
            go_up(round_z.at[1], round_z.at[1], round_recv.at[1]).wait_recv()
            go_up(round_z.at[1], round_z.at[1], round_recv.at[1]).start()

        @pl.when(gz == 2)
        def _():
            go_down(round_z.at[0], round_z.at[0], round_recv.at[0]).wait_recv()
            go_down(round_z.at[0], round_z.at[0], round_recv.at[0]).start()

    def z_pass_on():
        @pl.when(gz == 1)
        def _():
            go_down(round_z.at[0], round_z.at[0], round_recv.at[0]).wait_recv()
            go_down(round_z.at[0], z_before, z_recv).start()

        @pl.when(gz == 2)
        def _():
            go_up(round_z.at[1], round_z.at[1], round_recv.at[1]).wait_recv()
            go_up(round_z.at[1], z_after, z_recv).start()

    def z_turn(p, _):
        turned = jnp.transpose(xp[pl.ds(2 * p, 2), pl.ds(reach, cells)].reshape(128, 128))
        zt[p, 8:136] = turned
        for i in range(reach):
            edge[0, i, pl.ds(p, 1)] = turned[i : i + 1]
            edge[1, i, pl.ds(p, 1)] = turned[128 - reach + i : 129 - reach + i]
        return 0

    def y_turn(s, _):
        yt[s, pl.ds(reach, cells)] = jnp.swapaxes(xp[s, pl.ds(reach, cells)], 0, 1)
        return 0

    def z_sum(p, _):
        for i in range(reach):
            zt[p, 8 - reach + i : 9 - reach + i] = beside[0, i, pl.ds(p, 1)]
            zt[p, 136 + i : 137 + i] = beside[1, i, pl.ds(p, 1)]
        rows = []
        for r in range(16):
            at = 8 + 8 * r
            total = center * zt[p, at : at + 8]
            for k in range(1, reach + 1):
                total = total + weights[k - 1] * (zt[p, at - k : at - k + 8] + zt[p, at + k : at + k + 8])
            rows.append(total)
        acc[pl.ds(2 * p, 2)] = jnp.transpose(jnp.concatenate(rows, axis=0)).reshape(2, 8, 8, 128)
        return 0

    def y_sum(s, _):
        tiles = [yt[s, i] for i in range(cells + 2 * reach)]
        acc[s] = acc[s] + jnp.swapaxes(jnp.stack(tap_sum(tiles, cells), axis=0), 0, 1)
        return 0

    def finish(s, _):
        tiles = [xp[s, i] for i in range(cells + 2 * reach)]
        total = tap_sum(tiles, cells)
        factor = scale[s] * (1.0 / 1024.0)
        for x in range(cells):
            out[s, x] = tiles[reach + x] + factor * (total[x] + acc[s, x])
        return 0

    def relay(h):
        for j in range(chunks):
            if j < detour:

                @pl.when(jnp.logical_not(skips(h)))
                def _(j=j):
                    hop(h - 1, j).wait_recv()
                    hop(h, j).start()

            else:
                hop(h - 1, j).wait_recv()
                hop(h, j).start()

    with jax.named_scope("load_first"):
        loads[0].wait()
    with jax.named_scope("barrier_wait"):
        pl.semaphore_wait(barrier, greeted)

    @pl.when(downward & turns_round)
    def _():
        pl.semaphore_signal(round_go, inc=1, device_id=round_source, device_id_type=MESH)

    @pl.when(upward & sends_round)
    def _():
        pl.semaphore_signal(round_go, inc=1, device_id=round_turn, device_id_type=MESH)
        round_first().start()

    @pl.when(jnp.logical_not(sends_round))
    def _():
        for j in range(detour):
            hop(0, j).start()

    hop(0, 1).start()
    with jax.named_scope("load_rest"):
        loads[1].wait()
    hop(0, 2).start()
    with jax.named_scope("z_turn"):
        lax.fori_loop(0, pairs, z_turn, 0, unroll=2)
    with jax.named_scope("y_turn"):
        lax.fori_loop(0, species, y_turn, 0, unroll=2)
    with jax.named_scope("starts"):
        near.start()
        z_start()
        for j in range(3, chunks):
            hop(0, j).start()
        for copy in y_copies:
            copy.start()
    with jax.named_scope("relay1"):
        relay(1)
    with jax.named_scope("z_pass"):
        z_pass()
    with jax.named_scope("round_first"):

        @pl.when(downward & sends_round)
        def _():
            pl.semaphore_wait(round_go, 1)
            round_first().start()

    with jax.named_scope("relay2"):
        relay(2)
    with jax.named_scope("round_turn"):

        @pl.when(downward & turns_round)
        def _():
            pl.semaphore_wait(round_go, 1)

        @pl.when(turns_round)
        def _():
            round_first().wait_recv()
            round_last().start()

    with jax.named_scope("z_pass_on"):
        z_pass_on()
    with jax.named_scope("relay3"):
        relay(3)
    with jax.named_scope("z_wait"):
        z_both.wait_recv()
    with jax.named_scope("z_sum"):
        lax.fori_loop(0, pairs, z_sum, 0)
    with jax.named_scope("y_wait"):
        y_both.wait_recv()
    with jax.named_scope("y_sum"):
        lax.fori_loop(0, species, y_sum, 0)
    with jax.named_scope("near_wait"):
        near.wait()
        scale_copy.wait()
    with jax.named_scope("sent_wait"):
        y_both.wait_send()

        @pl.when(has_up)
        def _():
            z_sent[0].wait_send()

        @pl.when(has_down)
        def _():
            z_sent[1].wait_send()

    with jax.named_scope("finish"):
        for j in range(chunks):
            arrival(j).wait_recv()
            lax.fori_loop(j * per, (j + 1) * per, finish, 0)
    with jax.named_scope("send_wait"):
        hop(0, 0).wait_send()
        for h in range(1, relays + 1):

            @pl.when(jnp.logical_not(skips(h)))
            def _(h=h):
                hop(h, 0).wait_send()

        @pl.when(turns_round)
        def _():
            round_last().wait_send()

        rest = hold.at[:, pl.ds(detour * per, species - detour * per)]
        remote(rest, rest, x_send, far_recv.at[0], relay_to).wait_send()


def local(sizes, fields, strength):
    species, cells, rows, lanes = fields.shape
    return pl.pallas_call(
        functools.partial(kernel, sizes),
        out_shape=pltpu.VMEM(fields.shape, fields.dtype),
        in_specs=[pl.BlockSpec(memory_space=pl.ANY), pl.BlockSpec(memory_space=pl.ANY)],
        out_specs=pl.BlockSpec(memory_space=pltpu.VMEM),
        scratch_shapes=[
            pltpu.VMEM((species, cells + 2 * reach, rows, lanes), jnp.float32),
            pltpu.VMEM((species, rows + 2 * reach, cells, lanes), jnp.float32),
            pltpu.VMEM((species // 2, lanes + 16, 128), jnp.float32),
            pltpu.VMEM((species, cells, rows, lanes), jnp.float32),
            pltpu.VMEM((relays + 1, species, reach, rows, lanes), jnp.float32),
            pltpu.VMEM((2, reach, species // 2, 128), jnp.float32),
            pltpu.VMEM((2, reach, species // 2, 128), jnp.float32),
            pltpu.VMEM((2, reach, species // 2, 128), jnp.float32),
            pltpu.SMEM((species,), jnp.float32),
            pltpu.SemaphoreType.DMA((2,)),
            pltpu.SemaphoreType.DMA,
            pltpu.SemaphoreType.DMA,
            pltpu.SemaphoreType.DMA((relays + 2,)),
            pltpu.SemaphoreType.DMA((relays, chunks)),
            pltpu.SemaphoreType.DMA,
            pltpu.SemaphoreType.DMA((chunks,)),
            pltpu.SemaphoreType.DMA,
            pltpu.SemaphoreType.DMA,
            pltpu.SemaphoreType.DMA,
            pltpu.SemaphoreType.DMA,
            pltpu.SemaphoreType.DMA((2,)),
            pltpu.SemaphoreType.DMA,
            pltpu.SemaphoreType.DMA((2,)),
            pltpu.SemaphoreType.REGULAR,
        ],
        compiler_params=pltpu.CompilerParams(collective_id=0, has_side_effects=True),
    )(fields, strength)


def solution(mesh):
    sizes = (mesh.shape["gx"], mesh.shape["gy"], mesh.shape["gz"])
    return jax.shard_map(
        functools.partial(local, sizes),
        mesh=mesh,
        in_specs=(P(None, "gx", "gy", "gz"), P()),
        out_specs=P(None, "gx", "gy", "gz"),
        check_vma=False,
    )
```

```python
import functools

import jax
import jax.numpy as jnp
from jax import lax
from jax.experimental import pallas as pl
from jax.experimental.pallas import tpu as pltpu
from jax.sharding import PartitionSpec as P

MESH = pl.DeviceIdType.MESH

center = -252.0
weights = (210.0, -120.0, 45.0, -10.0, 1.0)
reach = 5

Z_GROUPS = 3
sizes_of_chunks = (4, 4, 4, 4, 4, 4, 4, 4)
chunks = len(sizes_of_chunks)
late = 3
relays = 3
detour = 1


def tap_sum(tiles, length):
    out = []
    for i in range(length):
        total = center * tiles[i + reach]
        for k in range(1, reach + 1):
            total = total + weights[k - 1] * (tiles[i + reach - k] + tiles[i + reach + k])
        out.append(total)
    return out


def kernel(
    sizes,
    fields,
    strength,
    out,
    xp,
    yt,
    zt,
    acc,
    hold,
    edge,
    beside,
    round_z,
    scale,
    load_sem,
    scale_sem,
    x_send,
    detour_send,
    late_send,
    hold_recv,
    detour_recv,
    far_recv,
    near_send,
    near_recv,
    y_send,
    y_recv,
    z_send,
    z_recv,
    round_recv,
    goes,
):
    nx, ny, nz = sizes
    species = xp.shape[0]
    cells = fields.shape[1]
    assert sum(sizes_of_chunks) == species
    at_chunk = [sum(sizes_of_chunks[:j]) for j in range(chunks + 1)]
    pairs = species // 2
    x_count = nx // (2 * Z_GROUPS)
    first = at_chunk[2]

    gx = lax.axis_index("gx")
    gy = lax.axis_index("gy")
    gz = lax.axis_index("gz")

    loads = [
        pltpu.make_async_copy(fields.at[pl.ds(at, n)], xp.at[pl.ds(at, n), pl.ds(reach, cells)], load_sem.at[i])
        for i, (at, n) in enumerate(((0, first), (first, species - first)))
    ]
    for copy in loads:
        copy.start()

    chip = lax.div(gx, 2)
    core = gx - 2 * chip
    chip_x = lax.div(chip, Z_GROUPS)
    z_hi = chip - Z_GROUPS * chip_x
    upward = core == 1
    downward = core == 0
    step = 2 * core - 1

    def wrap(v, n):
        return jnp.where(v < 0, v + n, jnp.where(v >= n, v - n, v))

    def along(d):
        lo = gz + d
        carry = jnp.where(lo < 0, -1, jnp.where(lo >= nz, 1, 0))
        return wrap(z_hi + carry, Z_GROUPS), lo - carry * nz

    def place(at_x, hi, lo, at_core):
        return {"gx": (at_x * Z_GROUPS + hi) * 2 + at_core, "gz": lo}

    ahead = along(step)
    behind = along(-step)
    crosses = jnp.where(upward, ahead[0] == 0, ahead[0] == Z_GROUPS - 1)
    relay_to = place(chip_x, *ahead, core)
    relay_from = place(chip_x, *behind, core)
    last_to = place(wrap(chip_x + jnp.where(crosses, step, 0), x_count), *ahead, 1 - core)
    crossed = jnp.where(upward, z_hi == Z_GROUPS - 1, z_hi == 0)
    last_from = place(wrap(chip_x + jnp.where(crossed, step, 0), x_count), *ahead, 1 - core)
    partner = {"gx": chip * 2 + 1 - core}
    y_up = {"gy": wrap(gy + 1, ny)}
    y_down = {"gy": wrap(gy - 1, ny)}
    z_up = {"gz": wrap(gz + 1, nz)}
    z_down = {"gz": wrap(gz - 1, nz)}
    has_up = gz < nz - 1
    has_down = gz > 0
    near_ahead = jnp.where(upward, gz < nz - 1, gz > 0)
    near_behind = jnp.where(upward, gz > 0, gz < nz - 1)

    bottom, middle, top = 0, Z_GROUPS - 2, Z_GROUPS - 1
    round_from = jnp.where(upward, top, bottom)
    round_to = top - round_from
    sends_round = z_hi == round_from
    turns_round = z_hi == middle
    beyond = wrap(chip_x + step, x_count) * Z_GROUPS
    round_mid = {"gx": (chip_x * Z_GROUPS + middle) * 2 + core}
    round_source = {"gx": (chip_x * Z_GROUPS + round_from) * 2 + core}
    round_end = {"gx": (beyond + round_to) * 2 + 1 - core}
    round_turn = {"gx": (beyond + middle) * 2 + 1 - core}
    round_ask = {"gx": (chip_x * Z_GROUPS + middle) * 2 + 1 - core}
    round_help = {"gx": (beyond + round_to) * 2 + core}
    round_tell = {"gx": (wrap(chip_x - step, x_count) * Z_GROUPS + middle) * 2 + core}
    round_tell_source = {"gx": (chip_x * Z_GROUPS + bottom) * 2 + 1 - core}
    gives_go = downward & (z_hi == top)

    def skips(h):
        below = jnp.where(gz < h, wrap(z_hi - 1, Z_GROUPS), z_hi)
        above = jnp.where(gz + h >= nz, wrap(z_hi + 1, Z_GROUPS), z_hi)
        return jnp.where(upward, below, above) == round_from

    sends_straight = upward & (z_hi == top) & (gz == nz - 1)
    gets_straight = downward & (z_hi == bottom) & (gz == nz - 1)
    straight_to = {"gx": (beyond + round_to) * 2 + 1 - core}
    straight_from = {"gx": (beyond + top) * 2 + 1 - core}

    def misses(h):
        return upward & (z_hi == bottom) & (gz == h - 1)

    barrier = pltpu.get_barrier_semaphore()

    def greet(who):
        pl.semaphore_signal(barrier, inc=1, device_id=who, device_id_type=MESH)

    for who in (relay_from, last_from, partner):
        greet(who)

    @pl.when(gy < ny - 1)
    def _():
        greet(y_up)

    @pl.when(gy == 0)
    def _():
        greet(y_down)

    @pl.when(upward & near_ahead)
    def _():
        greet(relay_to)

    @pl.when(upward & turns_round)
    def _():
        greet(round_source)

    @pl.when(downward & turns_round)
    def _():
        greet(round_help)

    @pl.when(downward & sends_round)
    def _():
        greet(round_ask)
        greet(round_turn)

    @pl.when(gets_straight)
    def _():
        greet(straight_from)

    also = jnp.where(sends_straight, 1, 0) + jnp.where(upward & near_behind, 1, 0) + jnp.where(gy == ny - 1, 2, jnp.where(gy > 0, 1, 0))
    greeted = 3 + also + jnp.where(upward & turns_round, 2, jnp.where(gives_go | (upward & sends_round), 1, 0))

    scale_copy = pltpu.make_async_copy(strength, scale, scale_sem)
    scale_copy.start()

    def part(j):
        return pl.ds(at_chunk[j], sizes_of_chunks[j])

    def remote(src, dst, send, recv, to):
        return pltpu.make_async_remote_copy(
            src_ref=src, dst_ref=dst, send_sem=send, recv_sem=recv, device_id=to, device_id_type=MESH
        )

    far_there = (reach + cells) * (1 - core)
    far_here = (reach + cells) * core

    def away(j):
        return xp.at[part(j), pl.ds(reach + (cells - reach) * core, reach)]

    def hop(h, j):
        src = away(j) if h == 0 else hold.at[h - 1, part(j)]
        send = detour_send.at[h] if j < detour else late_send.at[h] if j >= chunks - late else x_send
        if h < relays:
            return remote(src, hold.at[h, part(j)], send, hold_recv.at[h, j], relay_to)
        return remote(src, xp.at[part(j), pl.ds(far_there, reach)], send, far_recv.at[j], last_to)

    def arrival(j):
        return remote(hold.at[0, part(j)], xp.at[part(j), pl.ds(far_here, reach)], x_send, far_recv.at[j], last_to)

    def straight(j):
        dst = xp.at[part(j), pl.ds(far_there, reach)]
        return remote(away(j), dst, late_send.at[0], far_recv.at[j], straight_to)

    around = part(0)

    def round_first():
        src = xp.at[around, pl.ds(reach + (cells - reach) * core, reach)]
        return remote(src, hold.at[relays, around], detour_send.at[0], detour_recv, round_mid)

    def round_last():
        dst = xp.at[around, pl.ds(far_there, reach)]
        return remote(hold.at[relays, around], dst, detour_send.at[relays + 1], far_recv.at[0], round_end)

    near = remote(
        xp.at[:, pl.ds(reach + (cells - reach) * (1 - core), reach)],
        xp.at[:, pl.ds(far_here, reach)],
        near_send,
        near_recv,
        partner,
    )
    y_copies = (
        remote(yt.at[:, pl.ds(reach, reach)], yt.at[:, pl.ds(reach + cells, reach)], y_send, y_recv, y_down),
        remote(yt.at[:, pl.ds(cells, reach)], yt.at[:, pl.ds(0, reach)], y_send, y_recv, y_up),
    )
    y_both = remote(yt.at[:, pl.ds(0, 2 * reach)], yt.at[:, pl.ds(0, 2 * reach)], y_send, y_recv, y_up)

    z_first, z_last = edge.at[0], edge.at[1]
    z_before, z_after = beside.at[0], beside.at[1]
    z_both = remote(beside, beside, z_send.at[0], z_recv, z_up)
    z_sent = [remote(edge, edge, z_send.at[i], z_recv, z_up) for i in range(2)]

    def go_up(src, dst, recv):
        return remote(src, dst, z_send.at[0], recv, z_up)

    def go_down(src, dst, recv):
        return remote(src, dst, z_send.at[1], recv, z_down)

    def z_start():
        @pl.when(downward & has_up)
        def _():
            pl.semaphore_wait(goes.at[1], 1)

        @pl.when(has_up)
        def _():
            go_up(z_last, z_before, z_recv).start()

        @pl.when(has_down)
        def _():
            go_down(z_first, z_after, z_recv).start()

        @pl.when(gz == 0)
        def _():
            go_up(z_first, round_z.at[1], round_recv.at[1]).start()

        @pl.when(gz == nz - 1)
        def _():
            go_down(z_last, round_z.at[0], round_recv.at[0]).start()

    def z_pass():
        @pl.when(gz == 1)
        def _():
            go_up(round_z.at[1], round_z.at[1], round_recv.at[1]).wait_recv()
            go_up(round_z.at[1], round_z.at[1], round_recv.at[1]).start()

        @pl.when(gz == 2)
        def _():
            go_down(round_z.at[0], round_z.at[0], round_recv.at[0]).wait_recv()
            go_down(round_z.at[0], round_z.at[0], round_recv.at[0]).start()

    def z_pass_on():
        @pl.when(gz == 1)
        def _():
            go_down(round_z.at[0], round_z.at[0], round_recv.at[0]).wait_recv()
            go_down(round_z.at[0], z_before, z_recv).start()

        @pl.when(gz == 2)
        def _():
            go_up(round_z.at[1], round_z.at[1], round_recv.at[1]).wait_recv()
            go_up(round_z.at[1], z_after, z_recv).start()

    def z_turn(p, _):
        turned = jnp.transpose(xp[pl.ds(2 * p, 2), pl.ds(reach, cells)].reshape(128, 128))
        zt[p, 8:136] = turned
        for i in range(reach):
            edge[0, i, pl.ds(p, 1)] = turned[i : i + 1]
            edge[1, i, pl.ds(p, 1)] = turned[128 - reach + i : 129 - reach + i]
        return 0

    def y_turn(s, _):
        yt[s, pl.ds(reach, cells)] = jnp.swapaxes(xp[s, pl.ds(reach, cells)], 0, 1)
        return 0

    def z_sum(p, _):
        for i in range(reach):
            zt[p, 8 - reach + i : 9 - reach + i] = beside[0, i, pl.ds(p, 1)]
            zt[p, 136 + i : 137 + i] = beside[1, i, pl.ds(p, 1)]
        rows = []
        for r in range(16):
            at = 8 + 8 * r
            total = center * zt[p, at : at + 8]
            for k in range(1, reach + 1):
                total = total + weights[k - 1] * (zt[p, at - k : at - k + 8] + zt[p, at + k : at + k + 8])
            rows.append(total)
        acc[pl.ds(2 * p, 2)] = jnp.transpose(jnp.concatenate(rows, axis=0)).reshape(2, 8, 8, 128)
        return 0

    def y_sum(s, _):
        tiles = [yt[s, i] for i in range(cells + 2 * reach)]
        acc[s] = acc[s] + jnp.swapaxes(jnp.stack(tap_sum(tiles, cells), axis=0), 0, 1)
        return 0

    def finish(s, _):
        tiles = [xp[s, i] for i in range(cells + 2 * reach)]
        total = tap_sum(tiles, cells)
        factor = scale[s] * (1.0 / 1024.0)
        for x in range(cells):
            out[s, x] = tiles[reach + x] + factor * (total[x] + acc[s, x])
        return 0

    def relay(h):
        for j in range(chunks):
            if j < detour:

                @pl.when(jnp.logical_not(skips(h)))
                def _(j=j):
                    hop(h - 1, j).wait_recv()
                    hop(h, j).start()

            elif j < chunks - late:
                hop(h - 1, j).wait_recv()
                hop(h, j).start()

        @pl.when(jnp.logical_not(misses(h)))
        def _():
            for j in range(chunks - late, chunks):
                hop(h - 1, j).wait_recv()
                hop(h, j).start()

    with jax.named_scope("load_first"):
        loads[0].wait()
    with jax.named_scope("barrier_wait"):
        pl.semaphore_wait(barrier, greeted)

    @pl.when(upward & sends_round)
    def _():
        round_first().start()

    @pl.when(jnp.logical_not(sends_round))
    def _():
        for j in range(detour):
            hop(0, j).start()

    hop(0, 1).start()

    def go(i, who):
        pl.semaphore_signal(goes.at[i], inc=1, device_id=who, device_id_type=MESH)

    @pl.when(gives_go)
    def _():
        go(0, round_tell)

    @pl.when(upward & turns_round)
    def _():
        go(0, round_tell_source)

    @pl.when(downward & near_ahead)
    def _():
        go(1, relay_to)

    @pl.when(gy == ny - 1)
    def _():
        go(2, y_up)

    @pl.when(gy > 0)
    def _():
        go(2, y_down)

    with jax.named_scope("load_rest"):
        loads[1].wait()
    hop(0, 2).start()
    with jax.named_scope("z_turn"):
        lax.fori_loop(0, pairs, z_turn, 0, unroll=2)
    with jax.named_scope("y_turn"):
        lax.fori_loop(0, species, y_turn, 0, unroll=2)
    with jax.named_scope("starts"):
        near.start()
        z_start()
        for j in range(3, chunks - late):
            hop(0, j).start()

        @pl.when(jnp.logical_not(sends_straight))
        def _():
            for j in range(chunks - late, chunks):
                hop(0, j).start()


        @pl.when(gy < ny - 1)
        def _():
            pl.semaphore_wait(goes.at[2], jnp.where(gy == 0, 2, 1))

        for copy in y_copies:
            copy.start()
    with jax.named_scope("relay1"):
        relay(1)
    with jax.named_scope("z_pass"):
        z_pass()
    with jax.named_scope("round_first"):

        @pl.when(downward & sends_round)
        def _():
            pl.semaphore_wait(goes.at[0], 1)
            round_first().start()

    swaps = downward & (z_hi == bottom) & (gz == 1) & (chip_x == 0) & (gy == 0)
    with jax.named_scope("relay3_first"):

        @pl.when(swaps)
        def _():
            relay(3)

    with jax.named_scope("relay2"):
        relay(2)
    with jax.named_scope("round_turn"):

        @pl.when(downward & turns_round)
        def _():
            pl.semaphore_wait(goes.at[0], 1)

        @pl.when(turns_round)
        def _():
            round_first().wait_recv()
            round_last().start()

    with jax.named_scope("z_pass_on"):
        z_pass_on()
    with jax.named_scope("relay3"):

        @pl.when(jnp.logical_not(swaps))
        def _():
            relay(3)

        @pl.when(sends_straight)
        def _():
            for j in range(chunks - late, chunks):
                straight(j).start()

    with jax.named_scope("z_wait"):
        z_both.wait_recv()
    with jax.named_scope("z_sum"):
        lax.fori_loop(0, pairs, z_sum, 0)
    with jax.named_scope("y_wait"):
        y_both.wait_recv()
    with jax.named_scope("y_sum"):
        lax.fori_loop(0, species, y_sum, 0)
    with jax.named_scope("near_wait"):
        near.wait()
        scale_copy.wait()
    with jax.named_scope("sent_wait"):
        y_both.wait_send()

        @pl.when(has_up)
        def _():
            z_sent[0].wait_send()

        @pl.when(has_down)
        def _():
            z_sent[1].wait_send()

    with jax.named_scope("finish"):
        for j in range(chunks):
            arrival(j).wait_recv()
            lax.fori_loop(at_chunk[j], at_chunk[j + 1], finish, 0)
    with jax.named_scope("send_wait"):
        hop(0, 0).wait_send()
        for h in range(1, relays + 1):

            @pl.when(jnp.logical_not(skips(h)))
            def _(h=h):
                hop(h, 0).wait_send()

        @pl.when(turns_round)
        def _():
            round_last().wait_send()

        for h in range(relays + 1):
            end = hold.at[h, pl.ds(at_chunk[chunks - late], species - at_chunk[chunks - late])]

            @pl.when(jnp.logical_not(misses(h)) if h else h == 0)
            def _(h=h, end=end):
                remote(end, end, late_send.at[h], far_recv.at[0], relay_to).wait_send()

        rest = hold.at[:, pl.ds(at_chunk[1], at_chunk[chunks - late] - at_chunk[1])]
        remote(rest, rest, x_send, far_recv.at[0], relay_to).wait_send()


def local(sizes, fields, strength):
    species, cells, rows, lanes = fields.shape
    return pl.pallas_call(
        functools.partial(kernel, sizes),
        out_shape=pltpu.VMEM(fields.shape, fields.dtype),
        in_specs=[pl.BlockSpec(memory_space=pl.ANY), pl.BlockSpec(memory_space=pl.ANY)],
        out_specs=pl.BlockSpec(memory_space=pltpu.VMEM),
        scratch_shapes=[
            pltpu.VMEM((species, cells + 2 * reach, rows, lanes), jnp.float32),
            pltpu.VMEM((species, rows + 2 * reach, cells, lanes), jnp.float32),
            pltpu.VMEM((species // 2, lanes + 16, 128), jnp.float32),
            pltpu.VMEM((species, cells, rows, lanes), jnp.float32),
            pltpu.VMEM((relays + 1, species, reach, rows, lanes), jnp.float32),
            pltpu.VMEM((2, reach, species // 2, 128), jnp.float32),
            pltpu.VMEM((2, reach, species // 2, 128), jnp.float32),
            pltpu.VMEM((2, reach, species // 2, 128), jnp.float32),
            pltpu.SMEM((species,), jnp.float32),
            pltpu.SemaphoreType.DMA((2,)),
            pltpu.SemaphoreType.DMA,
            pltpu.SemaphoreType.DMA,
            pltpu.SemaphoreType.DMA((relays + 2,)),
            pltpu.SemaphoreType.DMA((relays + 1,)),
            pltpu.SemaphoreType.DMA((relays, chunks)),
            pltpu.SemaphoreType.DMA,
            pltpu.SemaphoreType.DMA((chunks,)),
            pltpu.SemaphoreType.DMA,
            pltpu.SemaphoreType.DMA,
            pltpu.SemaphoreType.DMA,
            pltpu.SemaphoreType.DMA,
            pltpu.SemaphoreType.DMA((2,)),
            pltpu.SemaphoreType.DMA,
            pltpu.SemaphoreType.DMA((2,)),
            pltpu.SemaphoreType.REGULAR((3,)),
        ],
        compiler_params=pltpu.CompilerParams(collective_id=0, has_side_effects=True),
    )(fields, strength)


def solution(mesh):
    sizes = (mesh.shape["gx"], mesh.shape["gy"], mesh.shape["gz"])
    return jax.shard_map(
        functools.partial(local, sizes),
        mesh=mesh,
        in_specs=(P(None, "gx", "gy", "gz"), P()),
        out_specs=P(None, "gx", "gy", "gz"),
        check_vma=False,
    )
```

```python
import functools

import jax
import jax.numpy as jnp
from jax import lax
from jax.experimental import pallas as pl
from jax.experimental.pallas import tpu as pltpu
from jax.sharding import PartitionSpec as P

MESH = pl.DeviceIdType.MESH

center = -252.0
weights = (210.0, -120.0, 45.0, -10.0, 1.0)
reach = 5

Z_GROUPS = 3
sizes_of_chunks = (4, 4, 4, 4, 4, 4, 4, 4)
chunks = len(sizes_of_chunks)
late = 2
relays = 3
detour = 3


def tap_sum(tiles, length):
    out = []
    for i in range(length):
        total = center * tiles[i + reach]
        for k in range(1, reach + 1):
            total = total + weights[k - 1] * (tiles[i + reach - k] + tiles[i + reach + k])
        out.append(total)
    return out


def kernel(
    sizes,
    fields,
    strength,
    out,
    xp,
    yt,
    zt,
    acc,
    hold,
    edge,
    beside,
    round_z,
    scale,
    load_sem,
    scale_sem,
    x_send,
    detour_send,
    second_send,
    late_send,
    hold_recv,
    detour_recv,
    far_recv,
    near_send,
    near_recv,
    y_send,
    y_recv,
    z_send,
    z_recv,
    round_recv,
    goes,
):
    nx, ny, nz = sizes
    species = xp.shape[0]
    cells = fields.shape[1]
    assert sum(sizes_of_chunks) == species
    at_chunk = [sum(sizes_of_chunks[:j]) for j in range(chunks + 1)]
    pairs = species // 2
    x_count = nx // (2 * Z_GROUPS)
    first = at_chunk[detour]

    gx = lax.axis_index("gx")
    gy = lax.axis_index("gy")
    gz = lax.axis_index("gz")

    loads = [
        pltpu.make_async_copy(fields.at[pl.ds(at, n)], xp.at[pl.ds(at, n), pl.ds(reach, cells)], load_sem.at[i])
        for i, (at, n) in enumerate(((0, first), (first, species - first)))
    ]
    for copy in loads:
        copy.start()

    chip = lax.div(gx, 2)
    core = gx - 2 * chip
    chip_x = lax.div(chip, Z_GROUPS)
    z_hi = chip - Z_GROUPS * chip_x
    upward = core == 1
    downward = core == 0
    step = 2 * core - 1

    def wrap(v, n):
        return jnp.where(v < 0, v + n, jnp.where(v >= n, v - n, v))

    def along(d):
        lo = gz + d
        carry = jnp.where(lo < 0, -1, jnp.where(lo >= nz, 1, 0))
        return wrap(z_hi + carry, Z_GROUPS), lo - carry * nz

    def place(at_x, hi, lo, at_core):
        return {"gx": (at_x * Z_GROUPS + hi) * 2 + at_core, "gz": lo}

    ahead = along(step)
    behind = along(-step)
    crosses = jnp.where(upward, ahead[0] == 0, ahead[0] == Z_GROUPS - 1)
    relay_to = place(chip_x, *ahead, core)
    relay_from = place(chip_x, *behind, core)
    last_to = place(wrap(chip_x + jnp.where(crosses, step, 0), x_count), *ahead, 1 - core)
    crossed = jnp.where(upward, z_hi == Z_GROUPS - 1, z_hi == 0)
    last_from = place(wrap(chip_x + jnp.where(crossed, step, 0), x_count), *ahead, 1 - core)
    partner = {"gx": chip * 2 + 1 - core}
    y_up = {"gy": wrap(gy + 1, ny)}
    y_down = {"gy": wrap(gy - 1, ny)}
    z_up = {"gz": wrap(gz + 1, nz)}
    z_down = {"gz": wrap(gz - 1, nz)}
    has_up = gz < nz - 1
    has_down = gz > 0
    near_ahead = jnp.where(upward, gz < nz - 1, gz > 0)
    near_behind = jnp.where(upward, gz > 0, gz < nz - 1)

    bottom, middle, top = 0, Z_GROUPS - 2, Z_GROUPS - 1
    round_from = jnp.where(upward, top, bottom)
    round_to = top - round_from
    lifts = gz >= nz // 2
    drops = (chip_x < x_count - 1) | (gy > 0) | (gz > 0)
    goes_round = jnp.where(upward, drops, lifts)
    sends_round = goes_round & (z_hi == round_from)
    turns_round = goes_round & (z_hi == middle)
    beyond = wrap(chip_x + step, x_count) * Z_GROUPS
    round_mid = {"gx": (chip_x * Z_GROUPS + middle) * 2 + core}
    round_source = {"gx": (chip_x * Z_GROUPS + round_from) * 2 + core}
    round_end = {"gx": (beyond + round_to) * 2 + 1 - core}
    round_turn = {"gx": (beyond + middle) * 2 + 1 - core}
    round_ask = {"gx": (chip_x * Z_GROUPS + middle) * 2 + 1 - core}
    round_help = {"gx": (beyond + round_to) * 2 + core}
    round_tell = {"gx": (wrap(chip_x - step, x_count) * Z_GROUPS + middle) * 2 + core}
    round_tell_source = {"gx": (chip_x * Z_GROUPS + bottom) * 2 + 1 - core}
    round_beside = {"gx": (chip_x * Z_GROUPS + top) * 2 + 1 - core}
    gives_go = downward & (z_hi == top)

    def skips(h):
        below = jnp.where(gz < h, wrap(z_hi - 1, Z_GROUPS), z_hi)
        above = jnp.where(gz + h >= nz, wrap(z_hi + 1, Z_GROUPS), z_hi)
        lo = jnp.where(gz + h >= nz, gz + h - nz, gz + h)
        from_lifted = (above == round_from) & (lo >= nz // 2)
        dropped = (below == round_from) & ((chip_x < x_count - 1) | (gy > 0) | (gz != h))
        return (upward & dropped) | (downward & from_lifted)

    def skipped(h, j):
        return skips(h) if j == 0 else downward & skips(h)

    sends_straight = upward & (z_hi == top) & (gz == nz - 1)
    gets_straight = downward & (z_hi == bottom) & (gz == nz - 1)
    straight_to = {"gx": (beyond + round_to) * 2 + 1 - core}
    straight_from = {"gx": (beyond + top) * 2 + 1 - core}

    def misses(h):
        return upward & (z_hi == bottom) & (gz == h - 1)

    barrier = pltpu.get_barrier_semaphore()

    def greet(who):
        pl.semaphore_signal(barrier, inc=1, device_id=who, device_id_type=MESH)

    for who in (relay_from, last_from, partner):
        greet(who)

    @pl.when(gy < ny - 1)
    def _():
        greet(y_up)

    @pl.when(gy == 0)
    def _():
        greet(y_down)

    @pl.when(upward & near_ahead)
    def _():
        greet(relay_to)

    @pl.when(upward & turns_round)
    def _():
        greet(round_beside)

    @pl.when(downward & turns_round)
    def _():
        greet(round_help)

    @pl.when(downward & (z_hi == bottom) & ((chip_x > 0) | (gy > 0) | (gz > 0)))
    def _():
        greet(round_turn)

    @pl.when(downward & sends_round)
    def _():
        greet(round_ask)

    @pl.when(gets_straight)
    def _():
        greet(straight_from)

    also = jnp.where(sends_straight, 1, 0) + jnp.where(upward & near_behind, 1, 0) + jnp.where(gy == ny - 1, 2, jnp.where(gy > 0, 1, 0))
    greeted = 3 + also + jnp.where(upward & turns_round, 1 + jnp.where(lifts, 1, 0), jnp.where(gives_go, jnp.where(drops, 1, 0) + jnp.where(lifts, 1, 0), 0))

    scale_copy = pltpu.make_async_copy(strength, scale, scale_sem)
    scale_copy.start()

    def part(j):
        return pl.ds(at_chunk[j], sizes_of_chunks[j])

    def remote(src, dst, send, recv, to):
        return pltpu.make_async_remote_copy(
            src_ref=src, dst_ref=dst, send_sem=send, recv_sem=recv, device_id=to, device_id_type=MESH
        )

    far_there = (reach + cells) * (1 - core)
    far_here = (reach + cells) * core

    def away(j):
        return xp.at[part(j), pl.ds(reach + (cells - reach) * core, reach)]

    def hop(h, j):
        src = away(j) if h == 0 else hold.at[h - 1, part(j)]
        send = x_send
        if j == 0:
            send = detour_send.at[h]
        elif j < detour:
            send = second_send.at[h]
        elif j >= chunks - late:
            send = late_send.at[h]
        if h < relays:
            return remote(src, hold.at[h, part(j)], send, hold_recv.at[h, j], relay_to)
        return remote(src, xp.at[part(j), pl.ds(far_there, reach)], send, far_recv.at[j], last_to)

    def arrival(j):
        return remote(hold.at[0, part(j)], xp.at[part(j), pl.ds(far_here, reach)], x_send, far_recv.at[j], last_to)

    def straight(j):
        dst = xp.at[part(j), pl.ds(far_there, reach)]
        return remote(away(j), dst, late_send.at[0], far_recv.at[j], straight_to)

    def around(ups):
        return pl.ds(0, at_chunk[detour if ups else 1])

    def round_first(ups):
        src = xp.at[around(ups), pl.ds(reach + (cells - reach) * core, reach)]
        return remote(src, hold.at[relays, around(ups)], detour_send.at[0], detour_recv, round_mid)

    def round_last(j):
        dst = xp.at[part(j), pl.ds(far_there, reach)]
        return remote(hold.at[relays, part(j)], dst, detour_send.at[relays + 1], far_recv.at[j], round_end)

    def round_done(ups):
        sent = hold.at[relays, around(ups)]
        return remote(sent, sent, detour_send.at[relays + 1], far_recv.at[0], round_end)

    near = remote(
        xp.at[:, pl.ds(reach + (cells - reach) * (1 - core), reach)],
        xp.at[:, pl.ds(far_here, reach)],
        near_send,
        near_recv,
        partner,
    )
    y_copies = (
        remote(yt.at[:, pl.ds(reach, reach)], yt.at[:, pl.ds(reach + cells, reach)], y_send, y_recv, y_down),
        remote(yt.at[:, pl.ds(cells, reach)], yt.at[:, pl.ds(0, reach)], y_send, y_recv, y_up),
    )
    y_both = remote(yt.at[:, pl.ds(0, 2 * reach)], yt.at[:, pl.ds(0, 2 * reach)], y_send, y_recv, y_up)

    z_first, z_last = edge.at[0], edge.at[1]
    z_before, z_after = beside.at[0], beside.at[1]
    z_both = remote(beside, beside, z_send.at[0], z_recv, z_up)
    z_sent = [remote(edge, edge, z_send.at[i], z_recv, z_up) for i in range(2)]

    def go_up(src, dst, recv):
        return remote(src, dst, z_send.at[0], recv, z_up)

    def go_down(src, dst, recv):
        return remote(src, dst, z_send.at[1], recv, z_down)

    def z_go_up():
        @pl.when(has_up)
        def _():
            go_up(z_last, z_before, z_recv).start()

        @pl.when(gz == 0)
        def _():
            go_up(z_first, round_z.at[1], round_recv.at[1]).start()

    def z_go_down():
        @pl.when(has_down)
        def _():
            go_down(z_first, z_after, z_recv).start()

        @pl.when(gz == nz - 1)
        def _():
            go_down(z_last, round_z.at[0], round_recv.at[0]).start()

    def z_pass():
        @pl.when(gz == 1)
        def _():
            go_up(round_z.at[1], round_z.at[1], round_recv.at[1]).wait_recv()
            go_up(round_z.at[1], round_z.at[1], round_recv.at[1]).start()

        @pl.when(gz == 2)
        def _():
            go_down(round_z.at[0], round_z.at[0], round_recv.at[0]).wait_recv()
            go_down(round_z.at[0], round_z.at[0], round_recv.at[0]).start()

    def z_pass_on():
        @pl.when(gz == 1)
        def _():
            go_down(round_z.at[0], round_z.at[0], round_recv.at[0]).wait_recv()
            go_down(round_z.at[0], z_before, z_recv).start()

        @pl.when(gz == 2)
        def _():
            go_up(round_z.at[1], round_z.at[1], round_recv.at[1]).wait_recv()
            go_up(round_z.at[1], z_after, z_recv).start()

    def z_turn(p, _):
        turned = jnp.transpose(xp[pl.ds(2 * p, 2), pl.ds(reach, cells)].reshape(128, 128))
        zt[p, 8:136] = turned
        for i in range(reach):
            edge[0, i, pl.ds(p, 1)] = turned[i : i + 1]
            edge[1, i, pl.ds(p, 1)] = turned[128 - reach + i : 129 - reach + i]
        return 0

    def y_turn(s, _):
        yt[s, pl.ds(reach, cells)] = jnp.swapaxes(xp[s, pl.ds(reach, cells)], 0, 1)
        return 0

    def z_sum(p, _):
        for i in range(reach):
            zt[p, 8 - reach + i : 9 - reach + i] = beside[0, i, pl.ds(p, 1)]
            zt[p, 136 + i : 137 + i] = beside[1, i, pl.ds(p, 1)]
        rows = []
        for r in range(16):
            at = 8 + 8 * r
            total = center * zt[p, at : at + 8]
            for k in range(1, reach + 1):
                total = total + weights[k - 1] * (zt[p, at - k : at - k + 8] + zt[p, at + k : at + k + 8])
            rows.append(total)
        acc[pl.ds(2 * p, 2)] = jnp.transpose(jnp.concatenate(rows, axis=0)).reshape(2, 8, 8, 128)
        return 0

    def y_sum(s, _):
        tiles = [yt[s, i] for i in range(cells + 2 * reach)]
        acc[s] = acc[s] + jnp.swapaxes(jnp.stack(tap_sum(tiles, cells), axis=0), 0, 1)
        return 0

    def finish(s, _):
        tiles = [xp[s, i] for i in range(cells + 2 * reach)]
        total = tap_sum(tiles, cells)
        factor = scale[s] * (1.0 / 1024.0)
        for x in range(cells):
            out[s, x] = tiles[reach + x] + factor * (total[x] + acc[s, x])
        return 0

    def relay(h):
        for j in range(chunks):
            if j < detour:

                @pl.when(jnp.logical_not(skipped(h, j)))
                def _(j=j):
                    hop(h - 1, j).wait_recv()
                    hop(h, j).start()

            elif j < chunks - late:
                hop(h - 1, j).wait_recv()
                hop(h, j).start()
            if h == 2 and j == detour:

                @pl.when(upward & turns_round)
                def _():
                    round_first(False).wait_recv()
                    round_last(0).start()


        @pl.when(jnp.logical_not(misses(h)))
        def _():
            for j in range(chunks - late, chunks):
                hop(h - 1, j).wait_recv()
                hop(h, j).start()

    with jax.named_scope("load_first"):
        loads[0].wait()
    with jax.named_scope("barrier_wait"):
        pl.semaphore_wait(barrier, greeted)

    for j in range(detour):

        @pl.when(jnp.logical_not(skipped(0, j)))
        def _(j=j):
            hop(0, j).start()

    def go(i, who):
        pl.semaphore_signal(goes.at[i], inc=1, device_id=who, device_id_type=MESH)

    @pl.when(gives_go & lifts)
    def _():
        go(0, round_tell)

    @pl.when(gives_go & drops)
    def _():
        go(0, partner)

    @pl.when(upward & turns_round & lifts)
    def _():
        go(0, round_tell_source)

    @pl.when(downward & near_ahead)
    def _():
        go(1, relay_to)

    @pl.when(gy == ny - 1)
    def _():
        go(2, y_up)

    @pl.when(gy > 0)
    def _():
        go(2, y_down)

    with jax.named_scope("load_rest"):
        loads[1].wait()
    hop(0, detour).start()
    with jax.named_scope("z_turn"):
        lax.fori_loop(0, pairs, z_turn, 0, unroll=2)
    with jax.named_scope("y_turn"):
        lax.fori_loop(0, species, y_turn, 0, unroll=2)
    with jax.named_scope("starts"):
        near.start()

        @pl.when(upward)
        def _():
            z_go_up()

        z_go_down()
        for j in range(detour + 1, chunks - late):
            hop(0, j).start()

        @pl.when(jnp.logical_not(sends_straight))
        def _():
            for j in range(chunks - late, chunks):
                hop(0, j).start()

        @pl.when(downward & has_up)
        def _():
            pl.semaphore_wait(goes.at[1], 1)
            z_go_up()

        @pl.when(upward & sends_round)
        def _():
            pl.semaphore_wait(goes.at[0], 1)
            round_first(False).start()

        @pl.when(gy < ny - 1)
        def _():
            pl.semaphore_wait(goes.at[2], jnp.where(gy == 0, 2, 1))

        for copy in y_copies:
            copy.start()
    with jax.named_scope("relay1"):
        relay(1)
    with jax.named_scope("z_pass"):
        z_pass()
    with jax.named_scope("round_first"):

        @pl.when(downward & sends_round)
        def _():
            pl.semaphore_wait(goes.at[0], 1)
            round_first(True).start()

    swaps = downward & (z_hi == bottom) & (gz == 1) & (chip_x == 0) & (gy == 0)
    with jax.named_scope("relay3_first"):

        @pl.when(swaps)
        def _():
            relay(3)

    with jax.named_scope("relay2"):
        relay(2)
    with jax.named_scope("round_turn"):

        @pl.when(downward & turns_round)
        def _():
            pl.semaphore_wait(goes.at[0], 1)
            round_first(True).wait_recv()
            for j in range(detour):
                round_last(j).start()

    with jax.named_scope("z_pass_on"):
        z_pass_on()
    with jax.named_scope("relay3"):

        @pl.when(jnp.logical_not(swaps))
        def _():
            relay(3)

        @pl.when(sends_straight)
        def _():
            for j in range(chunks - late, chunks):
                straight(j).start()

    with jax.named_scope("z_wait"):
        z_both.wait_recv()
    with jax.named_scope("z_sum"):
        lax.fori_loop(0, pairs, z_sum, 0)
    with jax.named_scope("y_wait"):
        y_both.wait_recv()
    with jax.named_scope("y_sum"):
        lax.fori_loop(0, species, y_sum, 0)
    with jax.named_scope("near_wait"):
        near.wait()
        scale_copy.wait()
    with jax.named_scope("finish"):
        for j in range(chunks):
            arrival(j).wait_recv()
            lax.fori_loop(at_chunk[j], at_chunk[j + 1], finish, 0)
    with jax.named_scope("sides_wait"):
        y_both.wait_send()

        @pl.when(has_up)
        def _():
            z_sent[0].wait_send()

        @pl.when(has_down)
        def _():
            z_sent[1].wait_send()

    with jax.named_scope("send_wait"):
        for ups in (False, True):

            @pl.when(sends_round & (downward if ups else upward))
            def _(ups=ups):
                round_first(ups).wait_send()

            @pl.when(turns_round & (downward if ups else upward))
            def _(ups=ups):
                round_done(ups).wait_send()

        for h in range(relays + 1):

            @pl.when(jnp.logical_not(skipped(h, 0)))
            def _(h=h):
                hop(h, 0).wait_send()

            @pl.when(jnp.logical_not(skipped(h, 1)))
            def _(h=h):
                more = hold.at[h, pl.ds(at_chunk[1], at_chunk[detour] - at_chunk[1])]
                remote(more, more, second_send.at[h], far_recv.at[0], relay_to).wait_send()

        for h in range(relays + 1):
            end = hold.at[h, pl.ds(at_chunk[chunks - late], species - at_chunk[chunks - late])]

            @pl.when(jnp.logical_not(misses(h)) if h else h == 0)
            def _(h=h, end=end):
                remote(end, end, late_send.at[h], far_recv.at[0], relay_to).wait_send()

        rest = hold.at[:, pl.ds(at_chunk[detour], at_chunk[chunks - late] - at_chunk[detour])]
        remote(rest, rest, x_send, far_recv.at[0], relay_to).wait_send()


def local(sizes, fields, strength):
    species, cells, rows, lanes = fields.shape
    return pl.pallas_call(
        functools.partial(kernel, sizes),
        out_shape=pltpu.VMEM(fields.shape, fields.dtype),
        in_specs=[pl.BlockSpec(memory_space=pl.ANY), pl.BlockSpec(memory_space=pl.ANY)],
        out_specs=pl.BlockSpec(memory_space=pltpu.VMEM),
        scratch_shapes=[
            pltpu.VMEM((species, cells + 2 * reach, rows, lanes), jnp.float32),
            pltpu.VMEM((species, rows + 2 * reach, cells, lanes), jnp.float32),
            pltpu.VMEM((species // 2, lanes + 16, 128), jnp.float32),
            pltpu.VMEM((species, cells, rows, lanes), jnp.float32),
            pltpu.VMEM((relays + 1, species, reach, rows, lanes), jnp.float32),
            pltpu.VMEM((2, reach, species // 2, 128), jnp.float32),
            pltpu.VMEM((2, reach, species // 2, 128), jnp.float32),
            pltpu.VMEM((2, reach, species // 2, 128), jnp.float32),
            pltpu.SMEM((species,), jnp.float32),
            pltpu.SemaphoreType.DMA((2,)),
            pltpu.SemaphoreType.DMA,
            pltpu.SemaphoreType.DMA,
            pltpu.SemaphoreType.DMA((relays + 2,)),
            pltpu.SemaphoreType.DMA((relays + 1,)),
            pltpu.SemaphoreType.DMA((relays + 1,)),
            pltpu.SemaphoreType.DMA((relays, chunks)),
            pltpu.SemaphoreType.DMA,
            pltpu.SemaphoreType.DMA((chunks,)),
            pltpu.SemaphoreType.DMA,
            pltpu.SemaphoreType.DMA,
            pltpu.SemaphoreType.DMA,
            pltpu.SemaphoreType.DMA,
            pltpu.SemaphoreType.DMA((2,)),
            pltpu.SemaphoreType.DMA,
            pltpu.SemaphoreType.DMA((2,)),
            pltpu.SemaphoreType.REGULAR((3,)),
        ],
        compiler_params=pltpu.CompilerParams(collective_id=0, has_side_effects=True),
    )(fields, strength)


def solution(mesh):
    sizes = (mesh.shape["gx"], mesh.shape["gy"], mesh.shape["gz"])
    return jax.shard_map(
        functools.partial(local, sizes),
        mesh=mesh,
        in_specs=(P(None, "gx", "gy", "gz"), P()),
        out_specs=P(None, "gx", "gy", "gz"),
        check_vma=False,
    )
```

```python
import functools

import jax
import jax.numpy as jnp
from jax import lax
from jax.experimental import pallas as pl
from jax.experimental.pallas import tpu as pltpu
from jax.sharding import PartitionSpec as P

MESH = pl.DeviceIdType.MESH

center = -252.0
weights = (210.0, -120.0, 45.0, -10.0, 1.0)
reach = 5

Z_GROUPS = 3
sizes_of_chunks = (4, 4, 4, 4, 4, 4, 4, 4)
chunks = len(sizes_of_chunks)
late = 2
straight_after = 3
relays = 3
detour = 3


def tap_sum(tiles, length):
    out = []
    for i in range(length):
        total = center * tiles[i + reach]
        for k in range(1, reach + 1):
            total = total + weights[k - 1] * (tiles[i + reach - k] + tiles[i + reach + k])
        out.append(total)
    return out


def kernel(
    sizes,
    fields,
    strength,
    out,
    xp,
    yt,
    zt,
    acc,
    hold,
    edge,
    beside,
    round_z,
    scale,
    load_sem,
    scale_sem,
    x_send,
    detour_send,
    second_send,
    late_send,
    hold_recv,
    detour_recv,
    far_recv,
    near_send,
    near_recv,
    y_send,
    y_recv,
    z_send,
    z_recv,
    round_recv,
    goes,
):
    nx, ny, nz = sizes
    species = xp.shape[0]
    cells = fields.shape[1]
    assert sum(sizes_of_chunks) == species
    at_chunk = [sum(sizes_of_chunks[:j]) for j in range(chunks + 1)]
    pairs = species // 2
    x_count = nx // (2 * Z_GROUPS)
    first = at_chunk[detour]

    gx = lax.axis_index("gx")
    gy = lax.axis_index("gy")
    gz = lax.axis_index("gz")

    loads = [
        pltpu.make_async_copy(fields.at[pl.ds(at, n)], xp.at[pl.ds(at, n), pl.ds(reach, cells)], load_sem.at[i])
        for i, (at, n) in enumerate(((0, first), (first, species - first)))
    ]
    for copy in loads:
        copy.start()

    chip = lax.div(gx, 2)
    core = gx - 2 * chip
    chip_x = lax.div(chip, Z_GROUPS)
    z_hi = chip - Z_GROUPS * chip_x
    upward = core == 1
    downward = core == 0
    step = 2 * core - 1

    def wrap(v, n):
        return jnp.where(v < 0, v + n, jnp.where(v >= n, v - n, v))

    def along(d):
        lo = gz + d
        carry = jnp.where(lo < 0, -1, jnp.where(lo >= nz, 1, 0))
        return wrap(z_hi + carry, Z_GROUPS), lo - carry * nz

    def place(at_x, hi, lo, at_core):
        return {"gx": (at_x * Z_GROUPS + hi) * 2 + at_core, "gz": lo}

    ahead = along(step)
    behind = along(-step)
    crosses = jnp.where(upward, ahead[0] == 0, ahead[0] == Z_GROUPS - 1)
    relay_to = place(chip_x, *ahead, core)
    relay_from = place(chip_x, *behind, core)
    last_to = place(wrap(chip_x + jnp.where(crosses, step, 0), x_count), *ahead, 1 - core)
    crossed = jnp.where(upward, z_hi == Z_GROUPS - 1, z_hi == 0)
    last_from = place(wrap(chip_x + jnp.where(crossed, step, 0), x_count), *ahead, 1 - core)
    partner = {"gx": chip * 2 + 1 - core}
    y_up = {"gy": wrap(gy + 1, ny)}
    y_down = {"gy": wrap(gy - 1, ny)}
    z_up = {"gz": wrap(gz + 1, nz)}
    z_down = {"gz": wrap(gz - 1, nz)}
    has_up = gz < nz - 1
    has_down = gz > 0
    near_ahead = jnp.where(upward, gz < nz - 1, gz > 0)
    near_behind = jnp.where(upward, gz > 0, gz < nz - 1)

    bottom, middle, top = 0, Z_GROUPS - 2, Z_GROUPS - 1
    round_from = jnp.where(upward, top, bottom)
    round_to = top - round_from
    lifts = gz >= nz // 2
    drops = (chip_x < x_count - 1) | (gy > 0) | (gz > 0)
    goes_round = jnp.where(upward, drops, lifts)
    sends_round = goes_round & (z_hi == round_from)
    turns_round = goes_round & (z_hi == middle)
    beyond = wrap(chip_x + step, x_count) * Z_GROUPS
    round_mid = {"gx": (chip_x * Z_GROUPS + middle) * 2 + core}
    round_source = {"gx": (chip_x * Z_GROUPS + round_from) * 2 + core}
    round_end = {"gx": (beyond + round_to) * 2 + 1 - core}
    round_turn = {"gx": (beyond + middle) * 2 + 1 - core}
    round_ask = {"gx": (chip_x * Z_GROUPS + middle) * 2 + 1 - core}
    round_help = {"gx": (beyond + round_to) * 2 + core}
    round_tell = {"gx": (wrap(chip_x - step, x_count) * Z_GROUPS + middle) * 2 + core}
    round_tell_source = {"gx": (chip_x * Z_GROUPS + bottom) * 2 + 1 - core}
    round_beside = {"gx": (chip_x * Z_GROUPS + top) * 2 + 1 - core}
    gives_go = downward & (z_hi == top)

    def skips(h):
        below = jnp.where(gz < h, wrap(z_hi - 1, Z_GROUPS), z_hi)
        above = jnp.where(gz + h >= nz, wrap(z_hi + 1, Z_GROUPS), z_hi)
        lo = jnp.where(gz + h >= nz, gz + h - nz, gz + h)
        from_lifted = (above == round_from) & (lo >= nz // 2)
        dropped = (below == round_from) & ((chip_x < x_count - 1) | (gy > 0) | (gz != h))
        return (upward & dropped) | (downward & from_lifted)

    def skipped(h, j):
        return skips(h) if j == 0 else downward & skips(h)

    straight_low = jnp.where((chip_x < x_count - 1) | (gy > 0), nz - 2, nz - 1)
    sends_straight = upward & (z_hi == top) & (gz >= straight_low)
    gets_straight = downward & (z_hi == bottom) & (gz >= jnp.where((chip_x > 0) | (gy > 0), nz - 2, nz - 1))
    straight_to = {"gx": (beyond + round_to) * 2 + 1 - core}
    straight_from = {"gx": (beyond + top) * 2 + 1 - core}

    def misses(h):
        hi = jnp.where(gz < h, wrap(z_hi - 1, Z_GROUPS), z_hi)
        lo = jnp.where(gz < h, gz - h + nz, gz - h)
        return upward & (hi == top) & (lo >= straight_low)

    barrier = pltpu.get_barrier_semaphore()

    def greet(who):
        pl.semaphore_signal(barrier, inc=1, device_id=who, device_id_type=MESH)

    for who in (relay_from, last_from, partner):
        greet(who)

    @pl.when(gy < ny - 1)
    def _():
        greet(y_up)

    @pl.when(gy == 0)
    def _():
        greet(y_down)

    @pl.when(upward & near_ahead)
    def _():
        greet(relay_to)

    @pl.when(upward & turns_round)
    def _():
        greet(round_beside)

    @pl.when(downward & turns_round)
    def _():
        greet(round_help)

    @pl.when(downward & (z_hi == bottom) & ((chip_x > 0) | (gy > 0) | (gz > 0)))
    def _():
        greet(round_turn)

    @pl.when(downward & sends_round)
    def _():
        greet(round_ask)

    @pl.when(gets_straight)
    def _():
        greet(straight_from)

    also = jnp.where(sends_straight, 1, 0) + jnp.where(upward & near_behind, 1, 0) + jnp.where(gy == ny - 1, 2, jnp.where(gy > 0, 1, 0))
    greeted = 3 + also + jnp.where(upward & turns_round, 1 + jnp.where(lifts, 1, 0), jnp.where(gives_go, jnp.where(drops, 1, 0) + jnp.where(lifts, 1, 0), 0))

    scale_copy = pltpu.make_async_copy(strength, scale, scale_sem)
    scale_copy.start()

    def part(j):
        return pl.ds(at_chunk[j], sizes_of_chunks[j])

    def remote(src, dst, send, recv, to):
        return pltpu.make_async_remote_copy(
            src_ref=src, dst_ref=dst, send_sem=send, recv_sem=recv, device_id=to, device_id_type=MESH
        )

    far_there = (reach + cells) * (1 - core)
    far_here = (reach + cells) * core

    def away(j):
        return xp.at[part(j), pl.ds(reach + (cells - reach) * core, reach)]

    def hop(h, j):
        src = away(j) if h == 0 else hold.at[h - 1, part(j)]
        send = x_send
        if j == 0:
            send = detour_send.at[h]
        elif j < detour:
            send = second_send.at[h]
        elif j >= chunks - late:
            send = late_send.at[h]
        if h < relays:
            return remote(src, hold.at[h, part(j)], send, hold_recv.at[h, j], relay_to)
        return remote(src, xp.at[part(j), pl.ds(far_there, reach)], send, far_recv.at[j], last_to)

    def arrival(j):
        return remote(hold.at[0, part(j)], xp.at[part(j), pl.ds(far_here, reach)], x_send, far_recv.at[j], last_to)

    def straight(j):
        dst = xp.at[part(j), pl.ds(far_there, reach)]
        return remote(away(j), dst, late_send.at[0], far_recv.at[j], straight_to)

    def around(ups):
        return pl.ds(0, at_chunk[detour if ups else 1])

    def round_first(ups):
        src = xp.at[around(ups), pl.ds(reach + (cells - reach) * core, reach)]
        return remote(src, hold.at[relays, around(ups)], detour_send.at[0], detour_recv, round_mid)

    def round_last(j):
        dst = xp.at[part(j), pl.ds(far_there, reach)]
        return remote(hold.at[relays, part(j)], dst, detour_send.at[relays + 1], far_recv.at[j], round_end)

    def round_done(ups):
        sent = hold.at[relays, around(ups)]
        return remote(sent, sent, detour_send.at[relays + 1], far_recv.at[0], round_end)

    near = remote(
        xp.at[:, pl.ds(reach + (cells - reach) * (1 - core), reach)],
        xp.at[:, pl.ds(far_here, reach)],
        near_send,
        near_recv,
        partner,
    )
    y_copies = (
        remote(yt.at[:, pl.ds(reach, reach)], yt.at[:, pl.ds(reach + cells, reach)], y_send, y_recv, y_down),
        remote(yt.at[:, pl.ds(cells, reach)], yt.at[:, pl.ds(0, reach)], y_send, y_recv, y_up),
    )
    y_both = remote(yt.at[:, pl.ds(0, 2 * reach)], yt.at[:, pl.ds(0, 2 * reach)], y_send, y_recv, y_up)

    z_first, z_last = edge.at[0], edge.at[1]
    z_before, z_after = beside.at[0], beside.at[1]
    z_both = remote(beside, beside, z_send.at[0], z_recv, z_up)
    z_sent = [remote(edge, edge, z_send.at[i], z_recv, z_up) for i in range(2)]

    def go_up(src, dst, recv):
        return remote(src, dst, z_send.at[0], recv, z_up)

    def go_down(src, dst, recv):
        return remote(src, dst, z_send.at[1], recv, z_down)

    def z_go_up():
        @pl.when(has_up)
        def _():
            go_up(z_last, z_before, z_recv).start()

        @pl.when(gz == 0)
        def _():
            go_up(z_first, round_z.at[1], round_recv.at[1]).start()

    def z_go_down():
        @pl.when(has_down)
        def _():
            go_down(z_first, z_after, z_recv).start()

        @pl.when(gz == nz - 1)
        def _():
            go_down(z_last, round_z.at[0], round_recv.at[0]).start()

    def z_pass():
        @pl.when(gz == 1)
        def _():
            go_up(round_z.at[1], round_z.at[1], round_recv.at[1]).wait_recv()
            go_up(round_z.at[1], round_z.at[1], round_recv.at[1]).start()

        @pl.when(gz == 2)
        def _():
            go_down(round_z.at[0], round_z.at[0], round_recv.at[0]).wait_recv()
            go_down(round_z.at[0], round_z.at[0], round_recv.at[0]).start()

    def z_pass_on():
        @pl.when(gz == 1)
        def _():
            go_down(round_z.at[0], round_z.at[0], round_recv.at[0]).wait_recv()
            go_down(round_z.at[0], z_before, z_recv).start()

        @pl.when(gz == 2)
        def _():
            go_up(round_z.at[1], round_z.at[1], round_recv.at[1]).wait_recv()
            go_up(round_z.at[1], z_after, z_recv).start()

    def z_turn(p, _):
        turned = jnp.transpose(xp[pl.ds(2 * p, 2), pl.ds(reach, cells)].reshape(128, 128))
        zt[p, 8:136] = turned
        for i in range(reach):
            edge[0, i, pl.ds(p, 1)] = turned[i : i + 1]
            edge[1, i, pl.ds(p, 1)] = turned[128 - reach + i : 129 - reach + i]
        return 0

    def y_turn(s, _):
        yt[s, pl.ds(reach, cells)] = jnp.swapaxes(xp[s, pl.ds(reach, cells)], 0, 1)
        return 0

    def z_sum(p, _):
        for i in range(reach):
            zt[p, 8 - reach + i : 9 - reach + i] = beside[0, i, pl.ds(p, 1)]
            zt[p, 136 + i : 137 + i] = beside[1, i, pl.ds(p, 1)]
        rows = []
        for r in range(16):
            at = 8 + 8 * r
            total = center * zt[p, at : at + 8]
            for k in range(1, reach + 1):
                total = total + weights[k - 1] * (zt[p, at - k : at - k + 8] + zt[p, at + k : at + k + 8])
            rows.append(total)
        acc[pl.ds(2 * p, 2)] = jnp.transpose(jnp.concatenate(rows, axis=0)).reshape(2, 8, 8, 128)
        return 0

    def y_sum(s, _):
        tiles = [yt[s, i] for i in range(cells + 2 * reach)]
        acc[s] = acc[s] + jnp.swapaxes(jnp.stack(tap_sum(tiles, cells), axis=0), 0, 1)
        return 0

    def finish(s, _):
        tiles = [xp[s, i] for i in range(cells + 2 * reach)]
        total = tap_sum(tiles, cells)
        factor = scale[s] * (1.0 / 1024.0)
        for x in range(cells):
            out[s, x] = tiles[reach + x] + factor * (total[x] + acc[s, x])
        return 0

    def go_straight():
        for j in range(chunks - late, chunks):
            straight(j).start()

    def relay(h):
        for j in range(chunks):
            if h == 3 and j == straight_after:

                @pl.when(sends_straight & (gz < nz - 1))
                def _():
                    go_straight()

            if j < detour:

                @pl.when(jnp.logical_not(skipped(h, j)))
                def _(j=j):
                    hop(h - 1, j).wait_recv()
                    hop(h, j).start()

            elif j < chunks - late:
                hop(h - 1, j).wait_recv()
                hop(h, j).start()
            if h == 2 and j == detour:

                @pl.when(upward & turns_round)
                def _():
                    round_first(False).wait_recv()
                    round_last(0).start()


        @pl.when(jnp.logical_not(misses(h)))
        def _():
            for j in range(chunks - late, chunks):
                hop(h - 1, j).wait_recv()
                hop(h, j).start()

    with jax.named_scope("load_first"):
        loads[0].wait()
    with jax.named_scope("barrier_wait"):
        pl.semaphore_wait(barrier, greeted)

    for j in range(detour):

        @pl.when(jnp.logical_not(skipped(0, j)))
        def _(j=j):
            hop(0, j).start()

    def go(i, who):
        pl.semaphore_signal(goes.at[i], inc=1, device_id=who, device_id_type=MESH)

    @pl.when(gives_go & lifts)
    def _():
        go(0, round_tell)

    @pl.when(gives_go & drops)
    def _():
        go(0, partner)

    @pl.when(upward & turns_round & lifts)
    def _():
        go(0, round_tell_source)

    @pl.when(downward & near_ahead)
    def _():
        go(1, relay_to)

    @pl.when(gy == ny - 1)
    def _():
        go(2, y_up)

    @pl.when(gy > 0)
    def _():
        go(2, y_down)

    with jax.named_scope("load_rest"):
        loads[1].wait()
    hop(0, detour).start()
    with jax.named_scope("z_turn"):
        lax.fori_loop(0, pairs, z_turn, 0, unroll=2)
    with jax.named_scope("y_turn"):
        lax.fori_loop(0, species, y_turn, 0, unroll=2)
    with jax.named_scope("starts"):
        near.start()

        @pl.when(upward)
        def _():
            z_go_up()

        z_go_down()
        for j in range(detour + 1, chunks - late):
            hop(0, j).start()

        @pl.when(jnp.logical_not(sends_straight))
        def _():
            for j in range(chunks - late, chunks):
                hop(0, j).start()

        @pl.when(downward & has_up)
        def _():
            pl.semaphore_wait(goes.at[1], 1)
            z_go_up()

        @pl.when(upward & sends_round)
        def _():
            pl.semaphore_wait(goes.at[0], 1)
            round_first(False).start()

        @pl.when(gy < ny - 1)
        def _():
            pl.semaphore_wait(goes.at[2], jnp.where(gy == 0, 2, 1))

        for copy in y_copies:
            copy.start()
    with jax.named_scope("relay1"):
        relay(1)
    with jax.named_scope("z_pass"):
        z_pass()
    with jax.named_scope("round_first"):

        @pl.when(downward & sends_round)
        def _():
            pl.semaphore_wait(goes.at[0], 1)
            round_first(True).start()

    swaps = downward & (z_hi == bottom) & (gz == 1) & (chip_x == 0) & (gy == 0)
    with jax.named_scope("relay3_first"):

        @pl.when(swaps)
        def _():
            relay(3)

    with jax.named_scope("relay2"):
        relay(2)
    with jax.named_scope("round_turn"):

        @pl.when(downward & turns_round)
        def _():
            pl.semaphore_wait(goes.at[0], 1)
            round_first(True).wait_recv()
            for j in range(detour):
                round_last(j).start()

    with jax.named_scope("z_pass_on"):
        z_pass_on()
    with jax.named_scope("relay3"):

        @pl.when(jnp.logical_not(swaps))
        def _():
            relay(3)

        @pl.when(sends_straight & (gz == nz - 1))
        def _():
            go_straight()

    with jax.named_scope("z_wait"):
        z_both.wait_recv()
    with jax.named_scope("z_sum"):
        lax.fori_loop(0, pairs, z_sum, 0)
    with jax.named_scope("y_wait"):
        y_both.wait_recv()
    with jax.named_scope("y_sum"):
        lax.fori_loop(0, species, y_sum, 0)
    with jax.named_scope("near_wait"):
        near.wait()
        scale_copy.wait()
    with jax.named_scope("finish"):
        for j in range(chunks):
            arrival(j).wait_recv()
            lax.fori_loop(at_chunk[j], at_chunk[j + 1], finish, 0)
    with jax.named_scope("sides_wait"):
        y_both.wait_send()

        @pl.when(has_up)
        def _():
            z_sent[0].wait_send()

        @pl.when(has_down)
        def _():
            z_sent[1].wait_send()

    with jax.named_scope("send_wait"):
        for ups in (False, True):

            @pl.when(sends_round & (downward if ups else upward))
            def _(ups=ups):
                round_first(ups).wait_send()

            @pl.when(turns_round & (downward if ups else upward))
            def _(ups=ups):
                round_done(ups).wait_send()

        for h in range(relays + 1):

            @pl.when(jnp.logical_not(skipped(h, 0)))
            def _(h=h):
                hop(h, 0).wait_send()

            @pl.when(jnp.logical_not(skipped(h, 1)))
            def _(h=h):
                more = hold.at[h, pl.ds(at_chunk[1], at_chunk[detour] - at_chunk[1])]
                remote(more, more, second_send.at[h], far_recv.at[0], relay_to).wait_send()

        for h in range(relays + 1):
            end = hold.at[h, pl.ds(at_chunk[chunks - late], species - at_chunk[chunks - late])]

            @pl.when(jnp.logical_not(misses(h)) if h else h == 0)
            def _(h=h, end=end):
                remote(end, end, late_send.at[h], far_recv.at[0], relay_to).wait_send()

        rest = hold.at[:, pl.ds(at_chunk[detour], at_chunk[chunks - late] - at_chunk[detour])]
        remote(rest, rest, x_send, far_recv.at[0], relay_to).wait_send()


def local(sizes, fields, strength):
    species, cells, rows, lanes = fields.shape
    return pl.pallas_call(
        functools.partial(kernel, sizes),
        out_shape=pltpu.VMEM(fields.shape, fields.dtype),
        in_specs=[pl.BlockSpec(memory_space=pl.ANY), pl.BlockSpec(memory_space=pl.ANY)],
        out_specs=pl.BlockSpec(memory_space=pltpu.VMEM),
        scratch_shapes=[
            pltpu.VMEM((species, cells + 2 * reach, rows, lanes), jnp.float32),
            pltpu.VMEM((species, rows + 2 * reach, cells, lanes), jnp.float32),
            pltpu.VMEM((species // 2, lanes + 16, 128), jnp.float32),
            pltpu.VMEM((species, cells, rows, lanes), jnp.float32),
            pltpu.VMEM((relays + 1, species, reach, rows, lanes), jnp.float32),
            pltpu.VMEM((2, reach, species // 2, 128), jnp.float32),
            pltpu.VMEM((2, reach, species // 2, 128), jnp.float32),
            pltpu.VMEM((2, reach, species // 2, 128), jnp.float32),
            pltpu.SMEM((species,), jnp.float32),
            pltpu.SemaphoreType.DMA((2,)),
            pltpu.SemaphoreType.DMA,
            pltpu.SemaphoreType.DMA,
            pltpu.SemaphoreType.DMA((relays + 2,)),
            pltpu.SemaphoreType.DMA((relays + 1,)),
            pltpu.SemaphoreType.DMA((relays + 1,)),
            pltpu.SemaphoreType.DMA((relays, chunks)),
            pltpu.SemaphoreType.DMA,
            pltpu.SemaphoreType.DMA((chunks,)),
            pltpu.SemaphoreType.DMA,
            pltpu.SemaphoreType.DMA,
            pltpu.SemaphoreType.DMA,
            pltpu.SemaphoreType.DMA,
            pltpu.SemaphoreType.DMA((2,)),
            pltpu.SemaphoreType.DMA,
            pltpu.SemaphoreType.DMA((2,)),
            pltpu.SemaphoreType.REGULAR((3,)),
        ],
        compiler_params=pltpu.CompilerParams(collective_id=0, has_side_effects=True),
    )(fields, strength)


def solution(mesh):
    sizes = (mesh.shape["gx"], mesh.shape["gy"], mesh.shape["gz"])
    return jax.shard_map(
        functools.partial(local, sizes),
        mesh=mesh,
        in_specs=(P(None, "gx", "gy", "gz"), P()),
        out_specs=P(None, "gx", "gy", "gz"),
        check_vma=False,
    )
```

```python
import functools

import jax
import jax.numpy as jnp
from jax import lax
from jax.experimental import pallas as pl
from jax.experimental.pallas import tpu as pltpu
from jax.sharding import PartitionSpec as P

MESH = pl.DeviceIdType.MESH

center = -252.0
weights = (210.0, -120.0, 45.0, -10.0, 1.0)
reach = 5

Z_GROUPS = 3
sizes_of_chunks = (4, 4, 4, 4, 4, 4, 4, 4)
chunks = len(sizes_of_chunks)
late = 2
straight_after = 3
relays = 3
detour = 3


def tap_sum(tiles, length):
    out = []
    for i in range(length):
        total = center * tiles[i + reach]
        for k in range(1, reach + 1):
            total = total + weights[k - 1] * (tiles[i + reach - k] + tiles[i + reach + k])
        out.append(total)
    return out


def kernel(
    sizes,
    fields,
    strength,
    out,
    xp,
    yt,
    zt,
    acc,
    hold,
    edge,
    beside,
    round_z,
    scale,
    load_sem,
    scale_sem,
    x_send,
    detour_send,
    second_send,
    late_send,
    hold_recv,
    detour_recv,
    far_recv,
    near_send,
    near_recv,
    y_send,
    y_recv,
    z_send,
    z_recv,
    round_recv,
    goes,
):
    nx, ny, nz = sizes
    species = xp.shape[0]
    cells = fields.shape[1]
    assert sum(sizes_of_chunks) == species
    at_chunk = [sum(sizes_of_chunks[:j]) for j in range(chunks + 1)]
    pairs = species // 2
    x_count = nx // (2 * Z_GROUPS)
    first = at_chunk[detour]

    gx = lax.axis_index("gx")
    gy = lax.axis_index("gy")
    gz = lax.axis_index("gz")

    loads = [
        pltpu.make_async_copy(fields.at[pl.ds(at, n)], xp.at[pl.ds(at, n), pl.ds(reach, cells)], load_sem.at[i])
        for i, (at, n) in enumerate(((0, first), (first, species - first)))
    ]
    for copy in loads:
        copy.start()

    chip = lax.div(gx, 2)
    core = gx - 2 * chip
    chip_x = lax.div(chip, Z_GROUPS)
    z_hi = chip - Z_GROUPS * chip_x
    upward = core == 1
    downward = core == 0
    step = 2 * core - 1

    def wrap(v, n):
        return jnp.where(v < 0, v + n, jnp.where(v >= n, v - n, v))

    def along(d):
        lo = gz + d
        carry = jnp.where(lo < 0, -1, jnp.where(lo >= nz, 1, 0))
        return wrap(z_hi + carry, Z_GROUPS), lo - carry * nz

    def place(at_x, hi, lo, at_core):
        return {"gx": (at_x * Z_GROUPS + hi) * 2 + at_core, "gz": lo}

    ahead = along(step)
    behind = along(-step)
    crosses = jnp.where(upward, ahead[0] == 0, ahead[0] == Z_GROUPS - 1)
    relay_to = place(chip_x, *ahead, core)
    relay_from = place(chip_x, *behind, core)
    last_to = place(wrap(chip_x + jnp.where(crosses, step, 0), x_count), *ahead, 1 - core)
    crossed = jnp.where(upward, z_hi == Z_GROUPS - 1, z_hi == 0)
    last_from = place(wrap(chip_x + jnp.where(crossed, step, 0), x_count), *ahead, 1 - core)
    partner = {"gx": chip * 2 + 1 - core}
    y_up = {"gy": wrap(gy + 1, ny)}
    y_down = {"gy": wrap(gy - 1, ny)}
    z_up = {"gz": wrap(gz + 1, nz)}
    z_down = {"gz": wrap(gz - 1, nz)}
    has_up = gz < nz - 1
    has_down = gz > 0
    near_ahead = jnp.where(upward, gz < nz - 1, gz > 0)
    near_behind = jnp.where(upward, gz > 0, gz < nz - 1)

    bottom, middle, top = 0, Z_GROUPS - 2, Z_GROUPS - 1
    round_from = jnp.where(upward, top, bottom)
    round_to = top - round_from
    lifts = gz >= nz // 2
    drops = (chip_x < x_count - 1) | (gy > 0) | (gz > 0)
    goes_round = jnp.where(upward, drops, lifts)
    sends_round = goes_round & (z_hi == round_from)
    turns_round = goes_round & (z_hi == middle)
    beyond = wrap(chip_x + step, x_count) * Z_GROUPS
    round_mid = {"gx": (chip_x * Z_GROUPS + middle) * 2 + core}
    round_source = {"gx": (chip_x * Z_GROUPS + round_from) * 2 + core}
    round_end = {"gx": (beyond + round_to) * 2 + 1 - core}
    round_turn = {"gx": (beyond + middle) * 2 + 1 - core}
    round_ask = {"gx": (chip_x * Z_GROUPS + middle) * 2 + 1 - core}
    round_help = {"gx": (beyond + round_to) * 2 + core}
    round_tell = {"gx": (wrap(chip_x - step, x_count) * Z_GROUPS + middle) * 2 + core}
    round_tell_source = {"gx": (chip_x * Z_GROUPS + bottom) * 2 + 1 - core}
    round_beside = {"gx": (chip_x * Z_GROUPS + top) * 2 + 1 - core}
    gives_go = downward & (z_hi == top)

    def skips(h):
        below = jnp.where(gz < h, wrap(z_hi - 1, Z_GROUPS), z_hi)
        above = jnp.where(gz + h >= nz, wrap(z_hi + 1, Z_GROUPS), z_hi)
        lo = jnp.where(gz + h >= nz, gz + h - nz, gz + h)
        from_lifted = (above == round_from) & (lo >= nz // 2)
        dropped = (below == round_from) & ((chip_x < x_count - 1) | (gy > 0) | (gz != h))
        return (upward & dropped) | (downward & from_lifted)

    def skipped(h, j):
        return skips(h) if j == 0 else downward & skips(h)

    straight_low = jnp.where((chip_x < x_count - 1) | (gy > 0), nz - 2, nz - 1)
    sends_straight = upward & (z_hi == top) & (gz >= straight_low)
    gets_straight = downward & (z_hi == bottom) & (gz >= jnp.where((chip_x > 0) | (gy > 0), nz - 2, nz - 1))
    straight_to = {"gx": (beyond + round_to) * 2 + 1 - core}
    straight_from = {"gx": (beyond + top) * 2 + 1 - core}

    def misses(h):
        hi = jnp.where(gz < h, wrap(z_hi - 1, Z_GROUPS), z_hi)
        lo = jnp.where(gz < h, gz - h + nz, gz - h)
        return upward & (hi == top) & (lo >= straight_low)

    barrier = pltpu.get_barrier_semaphore()

    def greet(who):
        pl.semaphore_signal(barrier, inc=1, device_id=who, device_id_type=MESH)

    for who in (relay_from, last_from, partner):
        greet(who)

    @pl.when(gy < ny - 1)
    def _():
        greet(y_up)

    @pl.when(gy == 0)
    def _():
        greet(y_down)

    @pl.when(upward & near_ahead)
    def _():
        greet(relay_to)

    @pl.when(upward & turns_round)
    def _():
        greet(round_beside)

    @pl.when(downward & turns_round)
    def _():
        greet(round_help)

    @pl.when(downward & (z_hi == bottom) & ((chip_x > 0) | (gy > 0) | (gz > 0)))
    def _():
        greet(round_turn)

    @pl.when(downward & sends_round)
    def _():
        greet(round_ask)

    @pl.when(gets_straight)
    def _():
        greet(straight_from)

    also = jnp.where(sends_straight, 1, 0) + jnp.where(upward & near_behind, 1, 0) + jnp.where(gy == ny - 1, 2, jnp.where(gy > 0, 1, 0))
    greeted = 3 + also + jnp.where(upward & turns_round, 1 + jnp.where(lifts, 1, 0), jnp.where(gives_go, jnp.where(drops, 1, 0) + jnp.where(lifts, 1, 0), 0))

    scale_copy = pltpu.make_async_copy(strength, scale, scale_sem)
    scale_copy.start()

    def part(j):
        return pl.ds(at_chunk[j], sizes_of_chunks[j])

    def remote(src, dst, send, recv, to):
        return pltpu.make_async_remote_copy(
            src_ref=src, dst_ref=dst, send_sem=send, recv_sem=recv, device_id=to, device_id_type=MESH
        )

    far_there = (reach + cells) * (1 - core)
    far_here = (reach + cells) * core

    def away(j):
        return xp.at[part(j), pl.ds(reach + (cells - reach) * core, reach)]

    def hop(h, j):
        src = away(j) if h == 0 else hold.at[h - 1, part(j)]
        send = x_send
        if j == 0:
            send = detour_send.at[h]
        elif j < detour:
            send = second_send.at[h]
        elif j >= chunks - late:
            send = late_send.at[h]
        if h < relays:
            return remote(src, hold.at[h, part(j)], send, hold_recv.at[h, j], relay_to)
        return remote(src, xp.at[part(j), pl.ds(far_there, reach)], send, far_recv.at[j], last_to)

    def arrival(j):
        return remote(hold.at[0, part(j)], xp.at[part(j), pl.ds(far_here, reach)], x_send, far_recv.at[j], last_to)

    def straight(j):
        dst = xp.at[part(j), pl.ds(far_there, reach)]
        return remote(away(j), dst, late_send.at[0], far_recv.at[j], straight_to)

    def around(ups):
        return pl.ds(0, at_chunk[detour if ups else 1])

    def round_first(ups):
        src = xp.at[around(ups), pl.ds(reach + (cells - reach) * core, reach)]
        return remote(src, hold.at[relays, around(ups)], detour_send.at[0], detour_recv, round_mid)

    def round_last(j):
        dst = xp.at[part(j), pl.ds(far_there, reach)]
        return remote(hold.at[relays, part(j)], dst, detour_send.at[relays + 1], far_recv.at[j], round_end)

    def round_done(ups):
        sent = hold.at[relays, around(ups)]
        return remote(sent, sent, detour_send.at[relays + 1], far_recv.at[0], round_end)

    near = remote(
        xp.at[:, pl.ds(reach + (cells - reach) * (1 - core), reach)],
        xp.at[:, pl.ds(far_here, reach)],
        near_send,
        near_recv,
        partner,
    )
    y_copies = (
        remote(yt.at[:, pl.ds(reach, reach)], yt.at[:, pl.ds(reach + cells, reach)], y_send, y_recv, y_down),
        remote(yt.at[:, pl.ds(cells, reach)], yt.at[:, pl.ds(0, reach)], y_send, y_recv, y_up),
    )
    y_both = remote(yt.at[:, pl.ds(0, 2 * reach)], yt.at[:, pl.ds(0, 2 * reach)], y_send, y_recv, y_up)

    z_first, z_last = edge.at[0], edge.at[1]
    z_before, z_after = beside.at[0], beside.at[1]
    z_both = remote(beside, beside, z_send.at[0], z_recv, z_up)
    z_sent = [remote(edge, edge, z_send.at[i], z_recv, z_up) for i in range(2)]

    def go_up(src, dst, recv):
        return remote(src, dst, z_send.at[0], recv, z_up)

    def go_down(src, dst, recv):
        return remote(src, dst, z_send.at[1], recv, z_down)

    def z_go_up():
        @pl.when(has_up)
        def _():
            go_up(z_last, z_before, z_recv).start()

        @pl.when(gz == 0)
        def _():
            go_up(z_first, round_z.at[1], round_recv.at[1]).start()

    def z_go_down():
        @pl.when(has_down)
        def _():
            go_down(z_first, z_after, z_recv).start()

        @pl.when(gz == nz - 1)
        def _():
            go_down(z_last, round_z.at[0], round_recv.at[0]).start()

    def z_pass():
        @pl.when(gz == 1)
        def _():
            go_up(round_z.at[1], round_z.at[1], round_recv.at[1]).wait_recv()
            go_up(round_z.at[1], round_z.at[1], round_recv.at[1]).start()

        @pl.when(gz == 2)
        def _():
            go_down(round_z.at[0], round_z.at[0], round_recv.at[0]).wait_recv()
            go_down(round_z.at[0], round_z.at[0], round_recv.at[0]).start()

    def z_pass_on():
        @pl.when(gz == 1)
        def _():
            go_down(round_z.at[0], round_z.at[0], round_recv.at[0]).wait_recv()
            go_down(round_z.at[0], z_before, z_recv).start()

        @pl.when(gz == 2)
        def _():
            go_up(round_z.at[1], round_z.at[1], round_recv.at[1]).wait_recv()
            go_up(round_z.at[1], z_after, z_recv).start()

    def z_turn(p, _):
        turned = jnp.transpose(xp[pl.ds(2 * p, 2), pl.ds(reach, cells)].reshape(128, 128))
        zt[p, 8:136] = turned
        for i in range(reach):
            edge[0, i, pl.ds(p, 1)] = turned[i : i + 1]
            edge[1, i, pl.ds(p, 1)] = turned[128 - reach + i : 129 - reach + i]
        return 0

    def y_turn(s, _):
        yt[s, pl.ds(reach, cells)] = jnp.swapaxes(xp[s, pl.ds(reach, cells)], 0, 1)
        return 0

    def z_sum(p, _):
        for i in range(reach):
            zt[p, 8 - reach + i : 9 - reach + i] = beside[0, i, pl.ds(p, 1)]
            zt[p, 136 + i : 137 + i] = beside[1, i, pl.ds(p, 1)]
        rows = []
        for r in range(16):
            at = 8 + 8 * r
            total = center * zt[p, at : at + 8]
            for k in range(1, reach + 1):
                total = total + weights[k - 1] * (zt[p, at - k : at - k + 8] + zt[p, at + k : at + k + 8])
            rows.append(total)
        acc[pl.ds(2 * p, 2)] = jnp.transpose(jnp.concatenate(rows, axis=0)).reshape(2, 8, 8, 128)
        return 0

    def y_sum(s, _):
        tiles = [yt[s, i] for i in range(cells + 2 * reach)]
        acc[s] = acc[s] + jnp.swapaxes(jnp.stack(tap_sum(tiles, cells), axis=0), 0, 1)
        return 0

    def finish(s, _):
        tiles = [xp[s, i] for i in range(cells + 2 * reach)]
        total = tap_sum(tiles, cells)
        factor = scale[s] * (1.0 / 1024.0)
        for x in range(cells):
            out[s, x] = tiles[reach + x] + factor * (total[x] + acc[s, x])
        return 0

    def go_straight():
        for j in range(chunks - late, chunks):
            straight(j).start()

    def relay(h):
        for j in range(chunks):
            if h == 3 and j == straight_after:

                @pl.when(sends_straight & (gz < nz - 1))
                def _():
                    go_straight()

            if j < detour:

                @pl.when(jnp.logical_not(skipped(h, j)))
                def _(j=j):
                    hop(h - 1, j).wait_recv()
                    hop(h, j).start()

            elif j < chunks - late:
                hop(h - 1, j).wait_recv()
                hop(h, j).start()
            if h == 2 and j == detour:

                @pl.when(upward & turns_round)
                def _():
                    round_first(False).wait_recv()
                    round_last(0).start()


        @pl.when(jnp.logical_not(misses(h)))
        def _():
            for j in range(chunks - late, chunks):
                hop(h - 1, j).wait_recv()
                hop(h, j).start()

    with jax.named_scope("load_first"):
        loads[0].wait()
    with jax.named_scope("barrier_wait"):
        pl.semaphore_wait(barrier, greeted)

    for j in range(detour):

        @pl.when(jnp.logical_not(skipped(0, j)))
        def _(j=j):
            hop(0, j).start()

    def go(i, who):
        pl.semaphore_signal(goes.at[i], inc=1, device_id=who, device_id_type=MESH)

    @pl.when(gives_go & lifts)
    def _():
        go(0, round_tell)

    @pl.when(gives_go & drops)
    def _():
        go(0, partner)

    @pl.when(upward & turns_round & lifts)
    def _():
        go(0, round_tell_source)

    @pl.when(downward & near_ahead)
    def _():
        go(1, relay_to)

    @pl.when(gy == ny - 1)
    def _():
        go(2, y_up)

    @pl.when(gy > 0)
    def _():
        go(2, y_down)

    with jax.named_scope("load_rest"):
        loads[1].wait()
    hop(0, detour).start()
    with jax.named_scope("z_turn"):
        lax.fori_loop(0, pairs, z_turn, 0, unroll=2)
    with jax.named_scope("y_turn"):
        lax.fori_loop(0, species, y_turn, 0, unroll=2)
    with jax.named_scope("starts"):
        near.start()

        @pl.when(upward)
        def _():
            z_go_up()

        z_go_down()
        for j in range(detour + 1, chunks - late):
            hop(0, j).start()

        @pl.when(jnp.logical_not(sends_straight))
        def _():
            for j in range(chunks - late, chunks):
                hop(0, j).start()

        @pl.when(downward & has_up)
        def _():
            pl.semaphore_wait(goes.at[1], 1)
            z_go_up()

        @pl.when(upward & sends_round)
        def _():
            pl.semaphore_wait(goes.at[0], 1)
            round_first(False).start()

        @pl.when(gy < ny - 1)
        def _():
            pl.semaphore_wait(goes.at[2], jnp.where(gy == 0, 2, 1))

        for copy in y_copies:
            copy.start()
    with jax.named_scope("relay1"):
        relay(1)
    with jax.named_scope("z_pass"):
        z_pass()
    with jax.named_scope("round_first"):

        @pl.when(downward & sends_round)
        def _():
            pl.semaphore_wait(goes.at[0], 1)
            round_first(True).start()

    swaps = downward & (z_hi == bottom) & (gz == 1) & (chip_x == 0) & (gy == 0)
    with jax.named_scope("relay3_first"):

        @pl.when(swaps)
        def _():
            relay(3)

    with jax.named_scope("relay2"):
        relay(2)
    with jax.named_scope("round_turn"):

        @pl.when(downward & turns_round)
        def _():
            pl.semaphore_wait(goes.at[0], 1)
            round_first(True).wait_recv()
            for j in range(detour):
                round_last(j).start()

    with jax.named_scope("z_pass_on"):
        z_pass_on()
    with jax.named_scope("relay3"):

        @pl.when(jnp.logical_not(swaps))
        def _():
            relay(3)

        @pl.when(sends_straight & (gz == nz - 1))
        def _():
            go_straight()

    with jax.named_scope("z_wait"):
        z_both.wait_recv()
    with jax.named_scope("z_sum"):
        lax.fori_loop(0, pairs, z_sum, 0)
    with jax.named_scope("y_wait"):
        y_both.wait_recv()
    with jax.named_scope("y_sum"):
        lax.fori_loop(0, species, y_sum, 0)
    with jax.named_scope("near_wait"):
        near.wait()
        scale_copy.wait()
    def wait_sent(h):
        @pl.when(jnp.logical_not(skipped(h, 0)))
        def _():
            hop(h, 0).wait_send()

        @pl.when(jnp.logical_not(skipped(h, 1)))
        def _():
            more = hold.at[h, pl.ds(at_chunk[1], at_chunk[detour] - at_chunk[1])]
            remote(more, more, second_send.at[h], far_recv.at[0], relay_to).wait_send()

        @pl.when(jnp.logical_not(misses(h)) if h else h == 0)
        def _():
            end = hold.at[h, pl.ds(at_chunk[chunks - late], species - at_chunk[chunks - late])]
            remote(end, end, late_send.at[h], far_recv.at[0], relay_to).wait_send()

    with jax.named_scope("finish"):
        for j in range(chunks):
            if j == chunks - 1:
                for h in range(relays):
                    if h:
                        wait_sent(h)
                y_both.wait_send()
            arrival(j).wait_recv()
            lax.fori_loop(at_chunk[j], at_chunk[j + 1], finish, 0)
    with jax.named_scope("send_wait"):

        @pl.when(has_up)
        def _():
            z_sent[0].wait_send()

        @pl.when(has_down)
        def _():
            z_sent[1].wait_send()

        for ups in (False, True):

            @pl.when(sends_round & (downward if ups else upward))
            def _(ups=ups):
                round_first(ups).wait_send()

            @pl.when(turns_round & (downward if ups else upward))
            def _(ups=ups):
                round_done(ups).wait_send()

        wait_sent(0)
        wait_sent(relays)
        rest = hold.at[:, pl.ds(at_chunk[detour], at_chunk[chunks - late] - at_chunk[detour])]
        remote(rest, rest, x_send, far_recv.at[0], relay_to).wait_send()


def local(sizes, fields, strength):
    species, cells, rows, lanes = fields.shape
    return pl.pallas_call(
        functools.partial(kernel, sizes),
        out_shape=pltpu.VMEM(fields.shape, fields.dtype),
        in_specs=[pl.BlockSpec(memory_space=pl.ANY), pl.BlockSpec(memory_space=pl.ANY)],
        out_specs=pl.BlockSpec(memory_space=pltpu.VMEM),
        scratch_shapes=[
            pltpu.VMEM((species, cells + 2 * reach, rows, lanes), jnp.float32),
            pltpu.VMEM((species, rows + 2 * reach, cells, lanes), jnp.float32),
            pltpu.VMEM((species // 2, lanes + 16, 128), jnp.float32),
            pltpu.VMEM((species, cells, rows, lanes), jnp.float32),
            pltpu.VMEM((relays + 1, species, reach, rows, lanes), jnp.float32),
            pltpu.VMEM((2, reach, species // 2, 128), jnp.float32),
            pltpu.VMEM((2, reach, species // 2, 128), jnp.float32),
            pltpu.VMEM((2, reach, species // 2, 128), jnp.float32),
            pltpu.SMEM((species,), jnp.float32),
            pltpu.SemaphoreType.DMA((2,)),
            pltpu.SemaphoreType.DMA,
            pltpu.SemaphoreType.DMA,
            pltpu.SemaphoreType.DMA((relays + 2,)),
            pltpu.SemaphoreType.DMA((relays + 1,)),
            pltpu.SemaphoreType.DMA((relays + 1,)),
            pltpu.SemaphoreType.DMA((relays, chunks)),
            pltpu.SemaphoreType.DMA,
            pltpu.SemaphoreType.DMA((chunks,)),
            pltpu.SemaphoreType.DMA,
            pltpu.SemaphoreType.DMA,
            pltpu.SemaphoreType.DMA,
            pltpu.SemaphoreType.DMA,
            pltpu.SemaphoreType.DMA((2,)),
            pltpu.SemaphoreType.DMA,
            pltpu.SemaphoreType.DMA((2,)),
            pltpu.SemaphoreType.REGULAR((3,)),
        ],
        compiler_params=pltpu.CompilerParams(collective_id=0, has_side_effects=True),
    )(fields, strength)


def solution(mesh):
    sizes = (mesh.shape["gx"], mesh.shape["gy"], mesh.shape["gz"])
    return jax.shard_map(
        functools.partial(local, sizes),
        mesh=mesh,
        in_specs=(P(None, "gx", "gy", "gz"), P()),
        out_specs=P(None, "gx", "gy", "gz"),
        check_vma=False,
    )
```

```python
import functools

import jax
import jax.numpy as jnp
from jax import lax
from jax.experimental import pallas as pl
from jax.experimental.pallas import tpu as pltpu
from jax.sharding import PartitionSpec as P

MESH = pl.DeviceIdType.MESH

center = -252.0
weights = (210.0, -120.0, 45.0, -10.0, 1.0)
reach = 5

Z_GROUPS = 3
sizes_of_chunks = (4, 4, 4, 4, 4, 4, 4, 4)
chunks = len(sizes_of_chunks)
late = 2
straight_after = 3
relays = 3
detour = 3


def tap_sum(tiles, length):
    out = []
    for i in range(length):
        total = center * tiles[i + reach]
        for k in range(1, reach + 1):
            total = total + weights[k - 1] * (tiles[i + reach - k] + tiles[i + reach + k])
        out.append(total)
    return out


def kernel(
    sizes,
    fields,
    strength,
    out,
    xp,
    yt,
    zt,
    acc,
    hold,
    edge,
    beside,
    round_z,
    scale,
    load_sem,
    scale_sem,
    sent,
    detour_send,
    hold_recv,
    detour_recv,
    far_recv,
    near_send,
    near_recv,
    y_send,
    y_recv,
    z_send,
    z_recv,
    round_recv,
    goes,
):
    nx, ny, nz = sizes
    species = xp.shape[0]
    cells = fields.shape[1]
    assert sum(sizes_of_chunks) == species
    assert sum(sizes_of_chunks[1:detour]) == sum(sizes_of_chunks[-late:])
    at_chunk = [sum(sizes_of_chunks[:j]) for j in range(chunks + 1)]
    pairs = species // 2
    x_count = nx // (2 * Z_GROUPS)
    first = at_chunk[detour]

    gx = lax.axis_index("gx")
    gy = lax.axis_index("gy")
    gz = lax.axis_index("gz")

    loads = [
        pltpu.make_async_copy(fields.at[pl.ds(at, n)], xp.at[pl.ds(at, n), pl.ds(reach, cells)], load_sem.at[i])
        for i, (at, n) in enumerate(((0, first), (first, species - first)))
    ]
    for copy in loads:
        copy.start()

    chip = lax.div(gx, 2)
    core = gx - 2 * chip
    chip_x = lax.div(chip, Z_GROUPS)
    z_hi = chip - Z_GROUPS * chip_x
    upward = core == 1
    downward = core == 0
    step = 2 * core - 1

    def wrap(v, n):
        return jnp.where(v < 0, v + n, jnp.where(v >= n, v - n, v))

    def along(d):
        lo = gz + d
        carry = jnp.where(lo < 0, -1, jnp.where(lo >= nz, 1, 0))
        return wrap(z_hi + carry, Z_GROUPS), lo - carry * nz

    def place(at_x, hi, lo, at_core):
        return {"gx": (at_x * Z_GROUPS + hi) * 2 + at_core, "gz": lo}

    ahead = along(step)
    behind = along(-step)
    crosses = jnp.where(upward, ahead[0] == 0, ahead[0] == Z_GROUPS - 1)
    relay_to = place(chip_x, *ahead, core)
    relay_from = place(chip_x, *behind, core)
    last_to = place(wrap(chip_x + jnp.where(crosses, step, 0), x_count), *ahead, 1 - core)
    crossed = jnp.where(upward, z_hi == Z_GROUPS - 1, z_hi == 0)
    last_from = place(wrap(chip_x + jnp.where(crossed, step, 0), x_count), *ahead, 1 - core)
    partner = {"gx": chip * 2 + 1 - core}
    y_up = {"gy": wrap(gy + 1, ny)}
    y_down = {"gy": wrap(gy - 1, ny)}
    z_up = {"gz": wrap(gz + 1, nz)}
    z_down = {"gz": wrap(gz - 1, nz)}
    has_up = gz < nz - 1
    has_down = gz > 0
    near_ahead = jnp.where(upward, gz < nz - 1, gz > 0)
    near_behind = jnp.where(upward, gz > 0, gz < nz - 1)

    bottom, middle, top = 0, Z_GROUPS - 2, Z_GROUPS - 1
    round_from = jnp.where(upward, top, bottom)
    round_to = top - round_from
    lifts = gz >= nz // 2
    drops = (chip_x < x_count - 1) | (gy > 0) | (gz > 0)
    goes_round = jnp.where(upward, drops, lifts)
    sends_round = goes_round & (z_hi == round_from)
    turns_round = goes_round & (z_hi == middle)
    beyond = wrap(chip_x + step, x_count) * Z_GROUPS
    round_mid = {"gx": (chip_x * Z_GROUPS + middle) * 2 + core}
    round_source = {"gx": (chip_x * Z_GROUPS + round_from) * 2 + core}
    round_end = {"gx": (beyond + round_to) * 2 + 1 - core}
    round_turn = {"gx": (beyond + middle) * 2 + 1 - core}
    round_ask = {"gx": (chip_x * Z_GROUPS + middle) * 2 + 1 - core}
    round_help = {"gx": (beyond + round_to) * 2 + core}
    round_tell = {"gx": (wrap(chip_x - step, x_count) * Z_GROUPS + middle) * 2 + core}
    round_tell_source = {"gx": (chip_x * Z_GROUPS + bottom) * 2 + 1 - core}
    round_beside = {"gx": (chip_x * Z_GROUPS + top) * 2 + 1 - core}
    gives_go = downward & (z_hi == top)

    def skips(h):
        below = jnp.where(gz < h, wrap(z_hi - 1, Z_GROUPS), z_hi)
        above = jnp.where(gz + h >= nz, wrap(z_hi + 1, Z_GROUPS), z_hi)
        lo = jnp.where(gz + h >= nz, gz + h - nz, gz + h)
        from_lifted = (above == round_from) & (lo >= nz // 2)
        dropped = (below == round_from) & ((chip_x < x_count - 1) | (gy > 0) | (gz != h))
        return (upward & dropped) | (downward & from_lifted)

    def skipped(h, j):
        return skips(h) if j == 0 else downward & skips(h)

    straight_low = jnp.where((chip_x < x_count - 1) | (gy > 0), nz - 2, nz - 1)
    sends_straight = upward & (z_hi == top) & (gz >= straight_low)
    gets_straight = downward & (z_hi == bottom) & (gz >= jnp.where((chip_x > 0) | (gy > 0), nz - 2, nz - 1))
    straight_to = {"gx": (beyond + round_to) * 2 + 1 - core}
    straight_from = {"gx": (beyond + top) * 2 + 1 - core}

    def misses(h):
        hi = jnp.where(gz < h, wrap(z_hi - 1, Z_GROUPS), z_hi)
        lo = jnp.where(gz < h, gz - h + nz, gz - h)
        return upward & (hi == top) & (lo >= straight_low)

    barrier = pltpu.get_barrier_semaphore()

    def greet(who):
        pl.semaphore_signal(barrier, inc=1, device_id=who, device_id_type=MESH)

    for who in (relay_from, last_from, partner):
        greet(who)

    @pl.when(gy < ny - 1)
    def _():
        greet(y_up)

    @pl.when(gy == 0)
    def _():
        greet(y_down)

    @pl.when(upward & near_ahead)
    def _():
        greet(relay_to)

    @pl.when(upward & turns_round)
    def _():
        greet(round_beside)

    @pl.when(downward & turns_round)
    def _():
        greet(round_help)

    @pl.when(downward & (z_hi == bottom) & ((chip_x > 0) | (gy > 0) | (gz > 0)))
    def _():
        greet(round_turn)

    @pl.when(downward & sends_round)
    def _():
        greet(round_ask)

    @pl.when(gets_straight)
    def _():
        greet(straight_from)

    also = jnp.where(sends_straight, 1, 0) + jnp.where(upward & near_behind, 1, 0) + jnp.where(gy == ny - 1, 2, jnp.where(gy > 0, 1, 0))
    greeted = 3 + also + jnp.where(upward & turns_round, 1 + jnp.where(lifts, 1, 0), jnp.where(gives_go, jnp.where(drops, 1, 0) + jnp.where(lifts, 1, 0), 0))

    scale_copy = pltpu.make_async_copy(strength, scale, scale_sem)
    scale_copy.start()

    def part(j):
        return pl.ds(at_chunk[j], sizes_of_chunks[j])

    def remote(src, dst, send, recv, to):
        return pltpu.make_async_remote_copy(
            src_ref=src, dst_ref=dst, send_sem=send, recv_sem=recv, device_id=to, device_id_type=MESH
        )

    far_there = (reach + cells) * (1 - core)
    far_here = (reach + cells) * core

    def away(j):
        return xp.at[part(j), pl.ds(reach + (cells - reach) * core, reach)]

    def hop(h, j):
        src = away(j) if h == 0 else hold.at[h - 1, part(j)]
        send = sent.at[relays + 1]
        if j == 0:
            send = detour_send.at[h]
        elif j < detour:
            send = sent.at[jnp.where(upward, relays + 1, h)]
        elif j >= chunks - late:
            send = sent.at[jnp.where(upward, h, relays + 1)]
        if h < relays:
            return remote(src, hold.at[h, part(j)], send, hold_recv.at[h, j], relay_to)
        return remote(src, xp.at[part(j), pl.ds(far_there, reach)], send, far_recv.at[j], last_to)

    def arrival(j):
        return remote(hold.at[0, part(j)], xp.at[part(j), pl.ds(far_here, reach)], sent.at[relays + 1], far_recv.at[j], last_to)

    def straight(j):
        dst = xp.at[part(j), pl.ds(far_there, reach)]
        return remote(away(j), dst, sent.at[0], far_recv.at[j], straight_to)

    def around(ups):
        return pl.ds(0, at_chunk[detour if ups else 1])

    def round_first(ups):
        src = xp.at[around(ups), pl.ds(reach + (cells - reach) * core, reach)]
        return remote(src, hold.at[relays, around(ups)], detour_send.at[0], detour_recv, round_mid)

    def round_last(j):
        dst = xp.at[part(j), pl.ds(far_there, reach)]
        return remote(hold.at[relays, part(j)], dst, detour_send.at[relays + 1], far_recv.at[j], round_end)

    def round_done(ups):
        done = hold.at[relays, around(ups)]
        return remote(done, done, detour_send.at[relays + 1], far_recv.at[0], round_end)

    near = remote(
        xp.at[:, pl.ds(reach + (cells - reach) * (1 - core), reach)],
        xp.at[:, pl.ds(far_here, reach)],
        near_send,
        near_recv,
        partner,
    )
    y_copies = (
        remote(yt.at[:, pl.ds(reach, reach)], yt.at[:, pl.ds(reach + cells, reach)], y_send, y_recv, y_down),
        remote(yt.at[:, pl.ds(cells, reach)], yt.at[:, pl.ds(0, reach)], y_send, y_recv, y_up),
    )
    y_both = remote(yt.at[:, pl.ds(0, 2 * reach)], yt.at[:, pl.ds(0, 2 * reach)], y_send, y_recv, y_up)

    z_first, z_last = edge.at[0], edge.at[1]
    z_before, z_after = beside.at[0], beside.at[1]
    z_both = remote(beside, beside, z_send.at[0], z_recv, z_up)
    z_sent = [remote(edge, edge, z_send.at[i], z_recv, z_up) for i in range(2)]

    def go_up(src, dst, recv):
        return remote(src, dst, z_send.at[0], recv, z_up)

    def go_down(src, dst, recv):
        return remote(src, dst, z_send.at[1], recv, z_down)

    def z_go_up():
        @pl.when(has_up)
        def _():
            go_up(z_last, z_before, z_recv).start()

        @pl.when(gz == 0)
        def _():
            go_up(z_first, round_z.at[1], round_recv.at[1]).start()

    def z_go_down():
        @pl.when(has_down)
        def _():
            go_down(z_first, z_after, z_recv).start()

        @pl.when(gz == nz - 1)
        def _():
            go_down(z_last, round_z.at[0], round_recv.at[0]).start()

    def z_pass():
        @pl.when(gz == 1)
        def _():
            go_up(round_z.at[1], round_z.at[1], round_recv.at[1]).wait_recv()
            go_up(round_z.at[1], round_z.at[1], round_recv.at[1]).start()

        @pl.when(gz == 2)
        def _():
            go_down(round_z.at[0], round_z.at[0], round_recv.at[0]).wait_recv()
            go_down(round_z.at[0], round_z.at[0], round_recv.at[0]).start()

    def z_pass_on():
        @pl.when(gz == 1)
        def _():
            go_down(round_z.at[0], round_z.at[0], round_recv.at[0]).wait_recv()
            go_down(round_z.at[0], z_before, z_recv).start()

        @pl.when(gz == 2)
        def _():
            go_up(round_z.at[1], round_z.at[1], round_recv.at[1]).wait_recv()
            go_up(round_z.at[1], z_after, z_recv).start()

    def z_turn(p, _):
        turned = jnp.transpose(xp[pl.ds(2 * p, 2), pl.ds(reach, cells)].reshape(128, 128))
        zt[p, 8:136] = turned
        for i in range(reach):
            edge[0, i, pl.ds(p, 1)] = turned[i : i + 1]
            edge[1, i, pl.ds(p, 1)] = turned[128 - reach + i : 129 - reach + i]
        return 0

    def y_turn(s, _):
        yt[s, pl.ds(reach, cells)] = jnp.swapaxes(xp[s, pl.ds(reach, cells)], 0, 1)
        return 0

    def z_sum(p, _):
        for i in range(reach):
            zt[p, 8 - reach + i : 9 - reach + i] = beside[0, i, pl.ds(p, 1)]
            zt[p, 136 + i : 137 + i] = beside[1, i, pl.ds(p, 1)]
        rows = []
        for r in range(16):
            at = 8 + 8 * r
            total = center * zt[p, at : at + 8]
            for k in range(1, reach + 1):
                total = total + weights[k - 1] * (zt[p, at - k : at - k + 8] + zt[p, at + k : at + k + 8])
            rows.append(total)
        acc[pl.ds(2 * p, 2)] = jnp.transpose(jnp.concatenate(rows, axis=0)).reshape(2, 8, 8, 128)
        return 0

    def y_sum(s, _):
        tiles = [yt[s, i] for i in range(cells + 2 * reach)]
        acc[s] = acc[s] + jnp.swapaxes(jnp.stack(tap_sum(tiles, cells), axis=0), 0, 1)
        return 0

    def finish(s, _):
        tiles = [xp[s, i] for i in range(cells + 2 * reach)]
        total = tap_sum(tiles, cells)
        factor = scale[s] * (1.0 / 1024.0)
        for x in range(cells):
            out[s, x] = tiles[reach + x] + factor * (total[x] + acc[s, x])
        return 0

    def go_straight():
        for j in range(chunks - late, chunks):
            straight(j).start()

    def relay(h):
        for j in range(chunks):
            if h == 3 and j == straight_after:

                @pl.when(sends_straight & (gz < nz - 1))
                def _():
                    go_straight()

            if j < detour:

                @pl.when(jnp.logical_not(skipped(h, j)))
                def _(j=j):
                    hop(h - 1, j).wait_recv()
                    hop(h, j).start()

            elif j < chunks - late:
                hop(h - 1, j).wait_recv()
                hop(h, j).start()
            if h == 2 and j == detour:

                @pl.when(upward & turns_round)
                def _():
                    round_first(False).wait_recv()
                    round_last(0).start()


        @pl.when(jnp.logical_not(misses(h)))
        def _():
            for j in range(chunks - late, chunks):
                hop(h - 1, j).wait_recv()
                hop(h, j).start()

    with jax.named_scope("load_first"):
        loads[0].wait()
    with jax.named_scope("barrier_wait"):
        pl.semaphore_wait(barrier, greeted)

    for j in range(detour):

        @pl.when(jnp.logical_not(skipped(0, j)))
        def _(j=j):
            hop(0, j).start()

    def go(i, who):
        pl.semaphore_signal(goes.at[i], inc=1, device_id=who, device_id_type=MESH)

    @pl.when(gives_go & lifts)
    def _():
        go(0, round_tell)

    @pl.when(gives_go & drops)
    def _():
        go(0, partner)

    @pl.when(upward & turns_round & lifts)
    def _():
        go(0, round_tell_source)

    @pl.when(downward & near_ahead)
    def _():
        go(1, relay_to)

    @pl.when(gy == ny - 1)
    def _():
        go(2, y_up)

    @pl.when(gy > 0)
    def _():
        go(2, y_down)

    with jax.named_scope("load_rest"):
        loads[1].wait()
    hop(0, detour).start()
    with jax.named_scope("z_turn"):
        lax.fori_loop(0, pairs, z_turn, 0, unroll=2)
    with jax.named_scope("y_turn"):
        lax.fori_loop(0, species, y_turn, 0, unroll=2)
    with jax.named_scope("starts"):
        near.start()

        @pl.when(upward)
        def _():
            z_go_up()

        z_go_down()
        for j in range(detour + 1, chunks - late):
            hop(0, j).start()

        @pl.when(jnp.logical_not(sends_straight))
        def _():
            for j in range(chunks - late, chunks):
                hop(0, j).start()

        @pl.when(downward & has_up)
        def _():
            pl.semaphore_wait(goes.at[1], 1)
            z_go_up()

        @pl.when(upward & sends_round)
        def _():
            pl.semaphore_wait(goes.at[0], 1)
            round_first(False).start()

        @pl.when(gy < ny - 1)
        def _():
            pl.semaphore_wait(goes.at[2], jnp.where(gy == 0, 2, 1))

        for copy in y_copies:
            copy.start()
    with jax.named_scope("relay1"):
        relay(1)
    with jax.named_scope("z_pass"):
        z_pass()
    with jax.named_scope("round_first"):

        @pl.when(downward & sends_round)
        def _():
            pl.semaphore_wait(goes.at[0], 1)
            round_first(True).start()

    swaps = downward & (z_hi == bottom) & (gz == 1) & (chip_x == 0) & (gy == 0)
    with jax.named_scope("relay3_first"):

        @pl.when(swaps)
        def _():
            relay(3)

    with jax.named_scope("relay2"):
        relay(2)
    with jax.named_scope("round_turn"):

        @pl.when(downward & turns_round)
        def _():
            pl.semaphore_wait(goes.at[0], 1)
            round_first(True).wait_recv()
            for j in range(detour):
                round_last(j).start()

    with jax.named_scope("z_pass_on"):
        z_pass_on()
    with jax.named_scope("relay3"):

        @pl.when(jnp.logical_not(swaps))
        def _():
            relay(3)

        @pl.when(sends_straight & (gz == nz - 1))
        def _():
            go_straight()

    with jax.named_scope("z_wait"):
        z_both.wait_recv()
    with jax.named_scope("z_sum"):
        lax.fori_loop(0, pairs, z_sum, 0)
    with jax.named_scope("y_wait"):
        y_both.wait_recv()
    with jax.named_scope("y_sum"):
        lax.fori_loop(0, species, y_sum, 0)
    with jax.named_scope("near_wait"):
        near.wait()
        scale_copy.wait()
    def wait_sent(h):
        @pl.when(jnp.logical_not(skipped(h, 0)))
        def _():
            hop(h, 0).wait_send()

        @pl.when(jnp.logical_not(misses(h) | skipped(h, 1) if h else skipped(h, 1)))
        def _():
            some = hold.at[h, pl.ds(0, at_chunk[detour] - at_chunk[1])]
            remote(some, some, sent.at[h], far_recv.at[0], relay_to).wait_send()

    with jax.named_scope("finish"):
        for j in range(chunks):
            if j == chunks - 1:
                for h in range(relays):
                    if h:
                        wait_sent(h)
                y_both.wait_send()
            arrival(j).wait_recv()
            lax.fori_loop(at_chunk[j], at_chunk[j + 1], finish, 0)
    with jax.named_scope("send_wait"):

        @pl.when(has_up)
        def _():
            z_sent[0].wait_send()

        @pl.when(has_down)
        def _():
            z_sent[1].wait_send()

        for ups in (False, True):

            @pl.when(sends_round & (downward if ups else upward))
            def _(ups=ups):
                round_first(ups).wait_send()

            @pl.when(turns_round & (downward if ups else upward))
            def _(ups=ups):
                round_done(ups).wait_send()

        wait_sent(0)
        wait_sent(relays)
        rest = hold.at[:, pl.ds(0, at_chunk[chunks - late] - at_chunk[1])]
        remote(rest, rest, sent.at[relays + 1], far_recv.at[0], relay_to).wait_send()


def local(sizes, fields, strength):
    species, cells, rows, lanes = fields.shape
    return pl.pallas_call(
        functools.partial(kernel, sizes),
        out_shape=pltpu.VMEM(fields.shape, fields.dtype),
        in_specs=[pl.BlockSpec(memory_space=pl.ANY), pl.BlockSpec(memory_space=pl.ANY)],
        out_specs=pl.BlockSpec(memory_space=pltpu.VMEM),
        scratch_shapes=[
            pltpu.VMEM((species, cells + 2 * reach, rows, lanes), jnp.float32),
            pltpu.VMEM((species, rows + 2 * reach, cells, lanes), jnp.float32),
            pltpu.VMEM((species // 2, lanes + 16, 128), jnp.float32),
            pltpu.VMEM((species, cells, rows, lanes), jnp.float32),
            pltpu.VMEM((relays + 1, species, reach, rows, lanes), jnp.float32),
            pltpu.VMEM((2, reach, species // 2, 128), jnp.float32),
            pltpu.VMEM((2, reach, species // 2, 128), jnp.float32),
            pltpu.VMEM((2, reach, species // 2, 128), jnp.float32),
            pltpu.SMEM((species,), jnp.float32),
            pltpu.SemaphoreType.DMA((2,)),
            pltpu.SemaphoreType.DMA,
            pltpu.SemaphoreType.DMA((relays + 2,)),
            pltpu.SemaphoreType.DMA((relays + 2,)),
            pltpu.SemaphoreType.DMA((relays, chunks)),
            pltpu.SemaphoreType.DMA,
            pltpu.SemaphoreType.DMA((chunks,)),
            pltpu.SemaphoreType.DMA,
            pltpu.SemaphoreType.DMA,
            pltpu.SemaphoreType.DMA,
            pltpu.SemaphoreType.DMA,
            pltpu.SemaphoreType.DMA((2,)),
            pltpu.SemaphoreType.DMA,
            pltpu.SemaphoreType.DMA((2,)),
            pltpu.SemaphoreType.REGULAR((3,)),
        ],
        compiler_params=pltpu.CompilerParams(collective_id=0, has_side_effects=True),
    )(fields, strength)


def solution(mesh):
    sizes = (mesh.shape["gx"], mesh.shape["gy"], mesh.shape["gz"])
    return jax.shard_map(
        functools.partial(local, sizes),
        mesh=mesh,
        in_specs=(P(None, "gx", "gy", "gz"), P()),
        out_specs=P(None, "gx", "gy", "gz"),
        check_vma=False,
    )
```
